32 devices in a mesh: mp: 4 (over x, core), batch: 8 (over z, y).
Axes of the slice: x: 2, y: 2, z: 4, core: 2. Of those that a mesh axis runs over, the one named last changes fastest.
Arguments:
- tokens: bfloat16 [16384, 768], P(('batch', 'mp')), may hold values from -6 to 6
- seg_ids: int32 [16384], P('batch'), may hold values from 0 to 17, as said below
- counts: int32 [8], P('batch'), may hold values from 128 to 2048, as said below
- gain_attn: float32 [768], replicated, may hold values from 0.5 to 1.5
- gain_ffn: float32 [768], replicated, may hold values from 0.5 to 1.5
- w_qkv: bfloat16 [768, 3, 768], P('batch', None, 'mp'), may hold values from -0.21875 to 0.21875
- dconv_kernel: float32 [3, 3, 768], P(None, None, 'mp'), may hold values from -3 to 3
- w_out: bfloat16 [768, 768], P('mp', 'batch'), may hold values from -1.75 to 1.75
- w_up: bfloat16 [768, 3072], P('batch', 'mp'), may hold values from -0.21875 to 0.21875
- w_down: bfloat16 [3072, 768], P('mp', 'batch'), may hold values from -0.109375 to 0.109375
- grad_out: bfloat16 [16384, 768], P(('batch', 'mp')), may hold values from -6 to 6
Outputs:
- layer_out: bfloat16 [16384, 768], P(('batch', 'mp'))
- grad_tokens: float32 [16384, 768], P(('batch', 'mp'))
- grad_gain_attn: float32 [768], P(('mp', 'batch'))
- grad_gain_ffn: float32 [768], P(('mp', 'batch'))
- grad_w_qkv: float32 [768, 3, 768], P('batch', None, 'mp')
- grad_dconv: float32 [3, 3, 768], P(None, None, ('mp', 'batch'))
- grad_w_out: float32 [768, 768], P('mp', 'batch')
- grad_w_up: float32 [768, 3072], P('batch', 'mp')
- grad_w_down: float32 [3072, 768], P('mp', 'batch')
The draws below stay inside these ranges and needn't reach their ends.
Inputs may be any that keep to these rules, and one draw needn't show every extreme that they name: `counts`: slots below a batch index's count are filled, the rest are empty; in every draw some batch index is full and some batch index holds a single sequence of exactly 128 slots. `seg_ids`: within a block of 2048 slots the ids never fall; each id of filled slots marks one sequence of 128 to 256 slots, except that a block's last sequence may be cut at the block's end; empty slots carry the id 2048 // 128 + 1, and some block has empty slots in every draw.
All inputs are finite; a program needn't handle non-finite values.
Results may differ from the reference program's by a relative error of at most 0.015.
Values may be sent and summed in bfloat16 or wider, within the bound.
A program may use at most 128 MiB of HBM per device.

```python
import jax
import jax.numpy as jnp
from jax import lax

D = 768
H = 12
HD = 64
FF = 3072
TOK_DEV = 2048
SEQ_MIN = 128
SEQ_MAX = 256
TOKENS = 16384
N_BATCH = 8


def packing(key):
    seq_slots = TOK_DEV // SEQ_MIN + 1
    lengths = jax.random.randint(jax.random.fold_in(key, 11), (N_BATCH, seq_slots), SEQ_MIN, SEQ_MAX + 1)
    used = jax.random.randint(jax.random.fold_in(key, 12), (N_BATCH,), 2, max(3, 2 * seq_slots // 3 + 1))
    full_index = jax.random.randint(jax.random.fold_in(key, 13), (), 0, N_BATCH)
    device_ids = lax.iota(jnp.int32, N_BATCH)
    single_row = device_ids == (full_index + 1) % N_BATCH
    first_column = lax.iota(jnp.int32, seq_slots) == 0
    lengths = jnp.where(single_row[:, None] & first_column[None, :], SEQ_MIN, lengths)
    ends = jnp.cumsum(lengths, axis=1).astype(jnp.int32)
    used = jnp.where(device_ids == full_index, seq_slots, used)
    used = jnp.where(single_row, 1, used)
    last_end = jnp.take_along_axis(ends, (used - 1)[:, None].astype(jnp.int32), axis=1)[:, 0]
    counts = jnp.minimum(last_end, TOK_DEV).astype(jnp.int32)
    slot_ids = lax.iota(jnp.int32, TOK_DEV)
    segment = jnp.sum((ends[:, None, :] <= slot_ids[None, :, None]).astype(jnp.int32), axis=-1)
    segment = jnp.where(slot_ids[None, :] < counts[:, None], segment, seq_slots).astype(jnp.int32)
    return (counts, segment.reshape(N_BATCH * TOK_DEV))


def draw_counts(key, part):
    return packing(key)[0]


def draw_seg_ids(key, part):
    return packing(key)[1]


def levels(stream_key, dims, cuts, smallest, largest):
    gain, own = 1.0, jax.random.fold_in(stream_key, 6)
    for axis_at, blocks in cuts:
        draws = jnp.exp(jax.random.uniform(jax.random.fold_in(own, axis_at), (blocks,), jnp.float32, smallest / len(cuts), largest / len(cuts)))
        gain = gain * jnp.repeat(draws, dims[axis_at] // blocks).reshape([-1 if axis == axis_at else 1 for axis in range(len(dims))])
    return gain


def centred(own_key, shape, spread, bound, shards=(), kind=jnp.bfloat16):
    loudness = levels(own_key, shape, shards, -0.22, 0.18) if shards else 1.0
    values = jax.random.normal(own_key, shape, jnp.float32) * spread * loudness
    return jnp.minimum(jnp.maximum(values, -bound), bound).astype(kind)


def setup_inputs(seed: int = 0) -> dict:
    keys = jax.random.split(jax.random.key(seed), 12)
    tokens = centred(keys[0], (TOKENS, D), 1.0, 6.0, ((0, 32),))
    seg_ids = draw_seg_ids(jax.random.fold_in(keys[11], 71), 0)
    counts = draw_counts(jax.random.fold_in(keys[11], 71), 0)
    gain_attn = jnp.clip(1.0 + 0.1 * jax.random.normal(keys[3], (D,), jnp.float32), 0.5, 1.5)
    gain_ffn = jnp.clip(1.0 + 0.1 * jax.random.normal(keys[4], (D,), jnp.float32), 0.5, 1.5)
    w_qkv = centred(keys[5], (D, 3, H * HD), D ** -0.5, 0.21875, ((0, 8), (2, 4)))
    dconv_kernel = centred(keys[6], (3, 3, H * HD), 0.6, 3.0, ((2, 4),), jnp.float32)
    w_out = centred(keys[7], (H * HD, D), (H * HD // 64) ** -0.5, 1.75, ((0, 4), (1, 8)))
    w_up = centred(keys[8], (D, FF), D ** -0.5, 0.21875, ((0, 8), (1, 4)))
    w_down = centred(keys[9], (FF, D), FF ** -0.5, 0.109375, ((0, 4), (1, 8)))
    grad_out = centred(keys[10], (TOKENS, D), 1.0, 6.0, ((0, 32),))
    return {"tokens": tokens, "seg_ids": seg_ids, "counts": counts, "gain_attn": gain_attn, "gain_ffn": gain_ffn, "w_qkv": w_qkv, "dconv_kernel": dconv_kernel, "w_out": w_out, "w_up": w_up, "w_down": w_down, "grad_out": grad_out}


EPSILON = 1e-06
MASKED = -1e+30

@jax.custom_vjp
def low(v):
    return lax.optimization_barrier(v.astype(jnp.bfloat16)).astype(jnp.float32)

@jax.custom_vjp
def low_back(v):
    return v

def low_keep(v):
    return (low(v), None)

def low_pass(kept, grad):
    return (grad,)

def back_keep(v):
    return (v, None)

def back_low(kept, grad):
    return (low(grad),)
low.defvjp(low_keep, low_pass)
low_back.defvjp(back_keep, back_low)

def rms_norm(values, gains):
    return values * lax.rsqrt(lax.optimization_barrier(jnp.mean(values * values, axis=-1, keepdims=True)) + EPSILON) * gains

def shifted(values, offset_by, filler):
    leading = jnp.full((offset_by,) + values.shape[1:], filler, values.dtype)
    return jnp.concatenate([leading, values[:-offset_by]], axis=0)

def same_masks(segment):
    segment = segment.astype(jnp.int32)
    same_one = (segment == shifted(segment, 1, -1)).astype(jnp.float32)[:, None, None]
    same_two = (segment == shifted(segment, 2, -1)).astype(jnp.float32)[:, None, None]
    return (same_one, same_two)

def depthwise(projected, kernel, same_one, same_two):
    return kernel[None, :, 0, :] * projected + kernel[None, :, 1, :] * shifted(projected, 1, 0.0) * same_one + kernel[None, :, 2, :] * shifted(projected, 2, 0.0) * same_two

def window(queries, keys_pad, values_pad, segment_pad, offset, block_rows, back_rows):
    q_block = lax.dynamic_slice_in_dim(queries, offset, block_rows, 0)
    k_block = lax.dynamic_slice_in_dim(keys_pad, offset, block_rows + back_rows, 0)
    v_block = lax.dynamic_slice_in_dim(values_pad, offset, block_rows + back_rows, 0)
    seg_query = lax.dynamic_slice_in_dim(segment_pad, offset + back_rows, block_rows, 0)
    seg_key = lax.dynamic_slice_in_dim(segment_pad, offset, block_rows + back_rows, 0)
    pos_query = offset + lax.iota(jnp.int32, block_rows)
    pos_key = offset - back_rows + lax.iota(jnp.int32, block_rows + back_rows)
    allowed = (seg_query[:, None] == seg_key[None, :]) & (pos_key[None, :] <= pos_query[:, None])
    return (q_block, k_block, v_block, allowed)

def attend(queries, keys_all, values_all, segment):
    row_count = queries.shape[0]
    block_rows = min(512, row_count)
    back_rows = SEQ_MAX
    scaling = queries.shape[-1] ** (-0.5)
    keys_pad = jnp.concatenate([jnp.zeros((back_rows,) + keys_all.shape[1:], keys_all.dtype), keys_all], axis=0)
    values_pad = jnp.concatenate([jnp.zeros((back_rows,) + values_all.shape[1:], values_all.dtype), values_all], axis=0)
    segment_pad = jnp.concatenate([jnp.full((back_rows,), -1, jnp.int32), segment.astype(jnp.int32)])

    def one_block(offset):
        q_block, k_block, v_block, allowed = window(queries, keys_pad, values_pad, segment_pad, offset, block_rows, back_rows)
        scores = jnp.einsum('qhd,khd->hqk', q_block, k_block, precision=lax.Precision.HIGHEST) * scaling
        scores = low_back(jnp.where(allowed[None], scores, MASKED))
        attn_prob = low(jax.nn.softmax(scores, axis=-1))
        return jnp.einsum('hqk,khd->qhd', attn_prob, v_block, precision=lax.Precision.HIGHEST)
    offsets = lax.iota(jnp.int32, row_count // block_rows) * block_rows
    outputs = lax.map(jax.checkpoint(one_block), offsets)
    return outputs.reshape(row_count, queries.shape[1], queries.shape[2])

def layer(params, tok_block, segment, filled):
    gain_attn, gain_ffn, w_qkv, kernel, w_out, w_up, w_down = params
    row_count = tok_block.shape[0]
    filled = filled[:, None]
    same_one, same_two = same_masks(segment)
    normed = low(rms_norm(tok_block, gain_attn))
    projected = low_back(jnp.einsum('td,dgc->tgc', normed, w_qkv, precision=lax.Precision.HIGHEST))
    mixed_qkv = low(depthwise(projected, kernel, same_one, same_two))
    mixed_qkv = mixed_qkv.reshape(row_count, 3, -1, HD)
    heads_out = low(low_back(attend(mixed_qkv[:, 0], mixed_qkv[:, 1], mixed_qkv[:, 2], segment)))
    attn_branch = low_back(jnp.dot(heads_out.reshape(row_count, -1), w_out, precision=lax.Precision.HIGHEST))
    residual = tok_block + filled * attn_branch
    normed_two = low(rms_norm(residual, gain_ffn))
    up_proj = low_back(jnp.dot(normed_two, w_up, precision=lax.Precision.HIGHEST))
    hidden = low(jnp.square(jax.nn.relu(up_proj)))
    ffn_branch = low_back(jnp.dot(hidden, w_down, precision=lax.Precision.HIGHEST))
    return residual + filled * ffn_branch

def reference(tokens, seg_ids, counts, gain_attn, gain_ffn, w_qkv, dconv_kernel, w_out, w_up, w_down, grad_out):
    slots = lax.iota(jnp.int32, TOK_DEV)
    filled = (slots[None, :] < counts.astype(jnp.int32)[:, None]).astype(jnp.float32)
    blocks = tokens.astype(jnp.float32).reshape(N_BATCH, TOK_DEV, D)
    segments = seg_ids.astype(jnp.int32).reshape(N_BATCH, TOK_DEV)
    params = (gain_attn.astype(jnp.float32), gain_ffn.astype(jnp.float32), w_qkv.astype(jnp.float32), dconv_kernel.astype(jnp.float32), w_out.astype(jnp.float32), w_up.astype(jnp.float32), w_down.astype(jnp.float32))

    def forward(weights, tok_blocks):

        def one_device(entry):
            return layer(weights, entry[0], entry[1], entry[2])
        return lax.map(jax.checkpoint(one_device), (tok_blocks, segments, filled))
    outputs, pull_back = jax.vjp(forward, params, blocks)
    grad_list, grad_blocks = pull_back(grad_out.astype(jnp.float32).reshape(N_BATCH, TOK_DEV, D))
    return (outputs.reshape(TOKENS, D).astype(jnp.bfloat16), grad_blocks.reshape(TOKENS, D), grad_list[0], grad_list[1], grad_list[2], grad_list[3], grad_list[4], grad_list[5], grad_list[6])
```

```python
import jax
import jax.numpy as jnp
from jax import lax
from jax.experimental import pallas as pl
from jax.experimental.pallas import tpu as pltpu
from jax.sharding import PartitionSpec as P

HD = 64
SEQ_MAX = 256
PAD = 16
EPSILON = 1e-06
MASKED = -1e30
F32 = jnp.float32
BF16 = jnp.bfloat16


def nt(left, right):
    return lax.dot_general(left, right, (((1,), (1,)), ((), ())), preferred_element_type=F32)


def nn(left, right):
    return lax.dot_general(left, right, (((1,), (0,)), ((), ())), preferred_element_type=F32)


def tn(left, right):
    return lax.dot_general(left, right, (((0,), (0,)), ((), ())), preferred_element_type=F32)


def head_mask(values, head):
    lane = lax.broadcasted_iota(jnp.int32, values.shape, 1)
    return jnp.where((lane >= head * HD) & (lane < (head + 1) * HD), values, jnp.zeros_like(values))


def attend_kernel(q_ref, k_ref, v_ref, seg_key_ref, seg_query_ref, out_ref, prob_ref, bias_ref):
    tile = SEQ_MAX
    tiles = q_ref.shape[0] // tile

    @pl.when(pl.program_id(0) == 0)
    def _():
        for at in range(tiles):
            key = lax.broadcasted_iota(jnp.int32, (2 * tile, tile), 0)
            query = lax.broadcasted_iota(jnp.int32, (2 * tile, tile), 1) + tile
            same = seg_key_ref[at * tile : (at + 2) * tile, :] == seg_query_ref[:, at * tile : (at + 1) * tile]
            bias_ref[at] = jnp.where(same & (key <= query), 0.0, MASKED).astype(F32)

    for at in range(tiles):
        keys = k_ref[at * tile : (at + 2) * tile, :]
        values = v_ref[at * tile : (at + 2) * tile, :]
        queries = q_ref[at * tile : (at + 1) * tile, :] * jnp.asarray(HD**-0.5, BF16)
        outs = []
        for head in range(2):
            scores = nt(keys, head_mask(queries, head)) + bias_ref[at]
            expo = jnp.exp(scores - jnp.max(scores, axis=0, keepdims=True))
            prob = (expo * (1.0 / jnp.sum(expo, axis=0, keepdims=True))).astype(BF16)
            prob_ref[0, at, head] = prob
            outs.append(tn(head_mask(values, head), prob))
        out_ref[at * tile : (at + 1) * tile, :] = (outs[0] + outs[1]).T.astype(BF16)


def attend_back_kernel(q_ref, k_ref, v_ref, grad_ref, prob_ref, dq_ref, dk_ref, dv_ref):
    tile = SEQ_MAX
    tiles = q_ref.shape[0] // tile
    dk_ref[...] = jnp.zeros_like(dk_ref)
    dv_ref[...] = jnp.zeros_like(dv_ref)
    for at in range(tiles):
        span = slice(at * tile, (at + 2) * tile)
        keys = k_ref[span, :]
        values = v_ref[span, :]
        queries = q_ref[at * tile : (at + 1) * tile, :] * jnp.asarray(HD**-0.5, BF16)
        grads = grad_ref[at * tile : (at + 1) * tile, :]
        dq = 0.0
        for head in range(2):
            prob = prob_ref[0, at, head]
            grad_head = head_mask(grads, head)
            grad_prob = nt(values, grad_head)
            wide = prob.astype(F32)
            inner = wide * grad_prob
            grad_scores = (inner - wide * jnp.sum(inner, axis=0, keepdims=True)).astype(BF16)
            dv_ref[span, :] += nn(prob, grad_head)
            dk_ref[span, :] += nn(grad_scores, head_mask(queries, head))
            dq = dq + tn(head_mask(keys, head), grad_scores)
        dq_ref[at * tile : (at + 1) * tile, :] = (dq * HD**-0.5).T


def attend(queries, keys, values, seg_key, seg_query):
    rows, width = queries.shape
    span = keys.shape[0]
    tiles = rows // SEQ_MAX
    wide = 2 * HD
    return pl.pallas_call(
        attend_kernel,
        grid=(width // wide,),
        in_specs=[
            pl.BlockSpec((rows, wide), lambda i: (0, i)),
            pl.BlockSpec((span, wide), lambda i: (0, i)),
            pl.BlockSpec((span, wide), lambda i: (0, i)),
            pl.BlockSpec((span, 1), lambda i: (0, 0)),
            pl.BlockSpec((1, rows), lambda i: (0, 0)),
        ],
        out_specs=[
            pl.BlockSpec((rows, wide), lambda i: (0, i)),
            pl.BlockSpec((1, tiles, 2, 2 * SEQ_MAX, SEQ_MAX), lambda i: (i, 0, 0, 0, 0)),
        ],
        out_shape=[
            jax.ShapeDtypeStruct((rows, width), BF16),
            jax.ShapeDtypeStruct((width // wide, tiles, 2, 2 * SEQ_MAX, SEQ_MAX), BF16),
        ],
        scratch_shapes=[pltpu.VMEM((tiles, 2 * SEQ_MAX, SEQ_MAX), F32)],
        name="attend",
    )(queries, keys, values, seg_key[:, None], seg_query[None, :])


def attend_back(queries, keys, values, grads, prob):
    rows, width = queries.shape
    span = keys.shape[0]
    tiles = rows // SEQ_MAX
    wide = 2 * HD
    return pl.pallas_call(
        attend_back_kernel,
        grid=(width // wide,),
        in_specs=[
            pl.BlockSpec((rows, wide), lambda i: (0, i)),
            pl.BlockSpec((span, wide), lambda i: (0, i)),
            pl.BlockSpec((span, wide), lambda i: (0, i)),
            pl.BlockSpec((rows, wide), lambda i: (0, i)),
            pl.BlockSpec((1, tiles, 2, 2 * SEQ_MAX, SEQ_MAX), lambda i: (i, 0, 0, 0, 0)),
        ],
        out_specs=[
            pl.BlockSpec((rows, wide), lambda i: (0, i)),
            pl.BlockSpec((span, wide), lambda i: (0, i)),
            pl.BlockSpec((span, wide), lambda i: (0, i)),
        ],
        out_shape=[
            jax.ShapeDtypeStruct((rows, width), F32),
            jax.ShapeDtypeStruct((span, width), F32),
            jax.ShapeDtypeStruct((span, width), F32),
        ],
        name="attend_back",
    )(queries, keys, values, grads, prob)


def rms(values):
    return lax.rsqrt(jnp.mean(values * values, axis=-1, keepdims=True) + EPSILON)


def rms_back(grad, gain, hat, scale):
    scaled = grad * gain
    return scale * (scaled - hat * jnp.mean(scaled * hat, axis=-1, keepdims=True))


def later(values, by):
    return jnp.concatenate([jnp.zeros((by,) + values.shape[1:], values.dtype), values[:-by]], axis=0)


def sooner(values, by):
    return jnp.concatenate([values[by:], jnp.zeros((by,) + values.shape[1:], values.dtype)], axis=0)


def shards(
    tokens, seg_ids, counts, gain_attn, gain_ffn, w_qkv, dconv_kernel, w_out, w_up, w_down, grad_out
):
    rows, width = tokens.shape
    halo = SEQ_MAX + PAD
    n_mp = lax.axis_size("mp")
    n_batch = lax.axis_size("batch")
    part = width // n_mp
    ff = w_up.shape[1] * n_mp
    own_start = lax.axis_index("mp") * rows

    packed = jnp.concatenate(
        [w_qkv.reshape(w_qkv.shape[0], -1), w_out.T, w_up, w_down.T], axis=1
    )
    full = lax.all_gather(packed, ("batch", "mp"), axis=0, tiled=False)
    full = full.reshape((n_batch, n_mp) + packed.shape).transpose(0, 2, 1, 3).reshape(width, n_mp, -1)
    cuts = (3 * part, 4 * part, 4 * part + w_up.shape[1])
    full_qkv = full[:, :, : cuts[0]].reshape(width, n_mp, 3, part).transpose(0, 2, 1, 3).reshape(width, 3 * width)
    full_out = full[:, :, cuts[0] : cuts[1]].reshape(width, width)
    full_up = full[:, :, cuts[1] : cuts[2]].reshape(width, ff)
    full_down = full[:, :, cuts[2] :].reshape(width, ff)
    kernel = lax.all_gather(dconv_kernel, "mp", axis=2, tiled=True).transpose(1, 0, 2).reshape(3, 3 * width)

    back = [(i, i + 1) for i in range(n_mp - 1)]
    tok_halo = lax.ppermute(tokens[rows - halo :], "mp", back)
    ext = jnp.concatenate([tok_halo, tokens], axis=0).astype(F32)
    seg_pad = jnp.concatenate([jnp.full((halo,), -1, jnp.int32), seg_ids])
    seg = lax.dynamic_slice_in_dim(seg_pad, own_start, halo + rows, 0)
    same_one = (seg == later(seg, 1)).astype(F32)[:, None]
    same_two = (seg == later(seg, 2)).astype(F32)[:, None]
    slot = own_start + lax.iota(jnp.int32, rows)
    filled = (slot < counts[0]).astype(F32)[:, None]

    scale_one = rms(ext)
    hat_one = ext * scale_one
    normed = (hat_one * gain_attn).astype(BF16)
    projected = nn(normed, full_qkv)
    mixed = (
        kernel[0] * projected
        + kernel[1] * same_one * later(projected, 1)
        + kernel[2] * same_two * later(projected, 2)
    ).astype(BF16)
    queries = mixed[halo:, :width]
    keys = mixed[PAD:, width : 2 * width]
    values = mixed[PAD:, 2 * width :]
    heads, prob = attend(queries, keys, values, seg[PAD:], seg[halo:])
    residual = ext[halo:] + filled * nn(heads, full_out.T if False else full_out.T)
    scale_two = rms(residual)
    hat_two = residual * scale_two
    normed_two = (hat_two * gain_ffn).astype(BF16)
    up = jax.nn.relu(nn(normed_two, full_up))
    hidden = (up * up).astype(BF16)
    layer_out = (residual + filled * nt(hidden, full_down)).astype(BF16)

    grad = grad_out.astype(F32)
    grad_ffn = (filled * grad).astype(BF16)
    grad_up = (nn(grad_ffn, full_down) * 2.0 * up).astype(BF16)
    grad_w_down = tn(grad_ffn, hidden)
    grad_w_up = tn(normed_two, grad_up)
    grad_normed_two = nt(grad_up, full_up)
    grad_resid = grad + rms_back(grad_normed_two, gain_ffn, hat_two, scale_two)
    grad_gain_ffn = jnp.sum(grad_normed_two * hat_two, axis=0)
    grad_attn = (filled * grad_resid).astype(BF16)
    grad_w_out = tn(grad_attn, heads)
    grad_heads = nn(grad_attn, full_out).astype(BF16)
    dq, dk, dv = attend_back(queries, keys, values, grad_heads, prob)
    grad_mixed = jnp.concatenate(
        [
            jnp.pad(dq, ((halo, 0), (0, 0))),
            jnp.pad(dk, ((PAD, 0), (0, 0))),
            jnp.pad(dv, ((PAD, 0), (0, 0))),
        ],
        axis=1,
    )
    one = grad_mixed * same_one
    two = grad_mixed * same_two
    grad_kernel = jnp.stack(
        [
            jnp.sum(grad_mixed * projected, axis=0),
            jnp.sum(one * later(projected, 1), axis=0),
            jnp.sum(two * later(projected, 2), axis=0),
        ]
    )
    grad_proj = (
        kernel[0] * grad_mixed + kernel[1] * sooner(one, 1) + kernel[2] * sooner(two, 2)
    ).astype(BF16)
    grad_w_qkv = tn(normed, grad_proj)
    grad_normed = nt(grad_proj, full_qkv)
    ahead = [(i + 1, i) for i in range(n_mp - 1)]
    passed = lax.ppermute(grad_normed[:halo].astype(BF16), "mp", ahead).astype(F32)
    own_normed = grad_normed[halo:] + jnp.pad(passed, ((rows - halo, 0), (0, 0)))
    grad_tokens = grad_resid + rms_back(own_normed, gain_attn, hat_one[halo:], scale_one[halo:])
    grad_gain_attn = jnp.sum(own_normed * hat_one[halo:], axis=0)

    shard = packed.shape[0]
    grads = jnp.concatenate(
        [
            grad_w_qkv.astype(BF16).reshape(width, 3, n_mp, part).transpose(0, 2, 1, 3).reshape(width, n_mp, -1),
            grad_w_out.astype(BF16).reshape(width, n_mp, -1),
            grad_w_up.astype(BF16).reshape(width, n_mp, -1),
            grad_w_down.astype(BF16).reshape(width, n_mp, -1),
        ],
        axis=2,
    )
    grads = grads.reshape(n_batch, shard, n_mp, -1).transpose(0, 2, 1, 3).reshape(n_batch * n_mp, shard, -1)
    own = lax.psum_scatter(grads, ("batch", "mp"), scatter_dimension=0, tiled=False).astype(F32)
    small = jnp.concatenate(
        [grad_kernel.reshape(3, 3, width).transpose(1, 0, 2).reshape(9, width), grad_gain_attn[None], grad_gain_ffn[None]]
    )
    piece = width // (n_mp * n_batch)
    small = small.reshape(11, n_mp * n_batch, piece).transpose(1, 0, 2)
    small = lax.psum_scatter(small, ("mp", "batch"), scatter_dimension=0, tiled=False)
    return (
        layer_out,
        grad_tokens,
        small[9],
        small[10],
        own[:, : cuts[0]].reshape(shard, 3, part),
        small[:9].reshape(3, 3, piece),
        own[:, cuts[0] : cuts[1]].T,
        own[:, cuts[1] : cuts[2]],
        own[:, cuts[2] :].T,
    )


def solution(mesh):
    in_specs = (
        P(("batch", "mp"), None),
        P("batch"),
        P("batch"),
        P(),
        P(),
        P("batch", None, "mp"),
        P(None, None, "mp"),
        P("mp", "batch"),
        P("batch", "mp"),
        P("mp", "batch"),
        P(("batch", "mp"), None),
    )
    out_specs = (
        P(("batch", "mp"), None),
        P(("batch", "mp"), None),
        P(("mp", "batch")),
        P(("mp", "batch")),
        P("batch", None, "mp"),
        P(None, None, ("mp", "batch")),
        P("mp", "batch"),
        P("batch", "mp"),
        P("mp", "batch"),
    )
    return jax.shard_map(shards, mesh=mesh, in_specs=in_specs, out_specs=out_specs, check_vma=False)
```

```python
import jax
import jax.numpy as jnp
from jax import lax
from jax.experimental import pallas as pl
from jax.experimental.pallas import tpu as pltpu
from jax.sharding import PartitionSpec as P

HD = 64
SEQ_MAX = 256
PAD = 16
EPSILON = 1e-06
MASKED = -1e30
F32 = jnp.float32
BF16 = jnp.bfloat16


def nt(left, right):
    return lax.dot_general(left, right, (((1,), (1,)), ((), ())), preferred_element_type=F32)


def nn(left, right):
    return lax.dot_general(left, right, (((1,), (0,)), ((), ())), preferred_element_type=F32)


def tn(left, right):
    return lax.dot_general(left, right, (((0,), (0,)), ((), ())), preferred_element_type=F32)


def head_mask(values, head):
    lane = lax.broadcasted_iota(jnp.int32, values.shape, 1)
    return jnp.where((lane >= head * HD) & (lane < (head + 1) * HD), values, jnp.zeros_like(values))


def attend_kernel(q_ref, k_ref, v_ref, seg_key_ref, seg_query_ref, out_ref, prob_ref, bias_ref):
    tile = SEQ_MAX
    tiles = q_ref.shape[0] // tile

    @pl.when(pl.program_id(0) == 0)
    def _():
        for at in range(tiles):
            key = lax.broadcasted_iota(jnp.int32, (2 * tile, tile), 0)
            query = lax.broadcasted_iota(jnp.int32, (2 * tile, tile), 1) + tile
            same = seg_key_ref[at * tile : (at + 2) * tile, :] == seg_query_ref[:, at * tile : (at + 1) * tile]
            bias_ref[at] = jnp.where(same & (key <= query), 0.0, MASKED).astype(F32)

    for at in range(tiles):
        keys = k_ref[at * tile : (at + 2) * tile, :]
        values = v_ref[at * tile : (at + 2) * tile, :]
        queries = q_ref[at * tile : (at + 1) * tile, :] * jnp.asarray(HD**-0.5, BF16)
        outs = []
        for head in range(2):
            scores = nt(keys, head_mask(queries, head)) + bias_ref[at]
            expo = jnp.exp(scores - jnp.max(scores, axis=0, keepdims=True))
            prob = (expo * (1.0 / jnp.sum(expo, axis=0, keepdims=True))).astype(BF16)
            prob_ref[0, at, head] = prob
            outs.append(tn(head_mask(values, head), prob))
        out_ref[at * tile : (at + 1) * tile, :] = (outs[0] + outs[1]).T.astype(BF16)


def attend_back_kernel(q_ref, k_ref, v_ref, grad_ref, prob_ref, dq_ref, dk_ref, dv_ref):
    tile = SEQ_MAX
    tiles = q_ref.shape[0] // tile
    dk_ref[...] = jnp.zeros_like(dk_ref)
    dv_ref[...] = jnp.zeros_like(dv_ref)
    for at in range(tiles):
        span = slice(at * tile, (at + 2) * tile)
        keys = k_ref[span, :]
        values = v_ref[span, :]
        queries = q_ref[at * tile : (at + 1) * tile, :] * jnp.asarray(HD**-0.5, BF16)
        grads = grad_ref[at * tile : (at + 1) * tile, :]
        dq = 0.0
        for head in range(2):
            prob = prob_ref[0, at, head]
            grad_head = head_mask(grads, head)
            grad_prob = nt(values, grad_head)
            wide = prob.astype(F32)
            inner = wide * grad_prob
            grad_scores = (inner - wide * jnp.sum(inner, axis=0, keepdims=True)).astype(BF16)
            dv_ref[span, :] += nn(prob, grad_head)
            dk_ref[span, :] += nn(grad_scores, head_mask(queries, head))
            dq = dq + tn(head_mask(keys, head), grad_scores)
        dq_ref[at * tile : (at + 1) * tile, :] = (dq * HD**-0.5).T


def attend(queries, keys, values, seg_key, seg_query):
    rows, width = queries.shape
    span = keys.shape[0]
    tiles = rows // SEQ_MAX
    wide = 2 * HD
    return pl.pallas_call(
        attend_kernel,
        grid=(width // wide,),
        in_specs=[
            pl.BlockSpec((rows, wide), lambda i: (0, i)),
            pl.BlockSpec((span, wide), lambda i: (0, i)),
            pl.BlockSpec((span, wide), lambda i: (0, i)),
            pl.BlockSpec((span, 1), lambda i: (0, 0)),
            pl.BlockSpec((1, rows), lambda i: (0, 0)),
        ],
        out_specs=[
            pl.BlockSpec((rows, wide), lambda i: (0, i)),
            pl.BlockSpec((1, tiles, 2, 2 * SEQ_MAX, SEQ_MAX), lambda i: (i, 0, 0, 0, 0)),
        ],
        out_shape=[
            jax.ShapeDtypeStruct((rows, width), BF16),
            jax.ShapeDtypeStruct((width // wide, tiles, 2, 2 * SEQ_MAX, SEQ_MAX), BF16),
        ],
        scratch_shapes=[pltpu.VMEM((tiles, 2 * SEQ_MAX, SEQ_MAX), F32)],
        name="attend",
    )(queries, keys, values, seg_key[:, None], seg_query[None, :])


def attend_back(queries, keys, values, grads, prob):
    rows, width = queries.shape
    span = keys.shape[0]
    tiles = rows // SEQ_MAX
    wide = 2 * HD
    return pl.pallas_call(
        attend_back_kernel,
        grid=(width // wide,),
        in_specs=[
            pl.BlockSpec((rows, wide), lambda i: (0, i)),
            pl.BlockSpec((span, wide), lambda i: (0, i)),
            pl.BlockSpec((span, wide), lambda i: (0, i)),
            pl.BlockSpec((rows, wide), lambda i: (0, i)),
            pl.BlockSpec((1, tiles, 2, 2 * SEQ_MAX, SEQ_MAX), lambda i: (i, 0, 0, 0, 0)),
        ],
        out_specs=[
            pl.BlockSpec((rows, wide), lambda i: (0, i)),
            pl.BlockSpec((span, wide), lambda i: (0, i)),
            pl.BlockSpec((span, wide), lambda i: (0, i)),
        ],
        out_shape=[
            jax.ShapeDtypeStruct((rows, width), F32),
            jax.ShapeDtypeStruct((span, width), F32),
            jax.ShapeDtypeStruct((span, width), F32),
        ],
        name="attend_back",
    )(queries, keys, values, grads, prob)


def rms(values):
    return lax.rsqrt(jnp.mean(values * values, axis=-1, keepdims=True) + EPSILON)


def rms_back(grad, gain, hat, scale):
    scaled = grad * gain
    return scale * (scaled - hat * jnp.mean(scaled * hat, axis=-1, keepdims=True))


def later(values, by):
    return jnp.concatenate([jnp.zeros((by,) + values.shape[1:], values.dtype), values[:-by]], axis=0)


def sooner(values, by):
    return jnp.concatenate([values[by:], jnp.zeros((by,) + values.shape[1:], values.dtype)], axis=0)


def shards_plain(
    tokens, seg_ids, counts, gain_attn, gain_ffn, w_qkv, dconv_kernel, w_out, w_up, w_down, grad_out
):
    rows, width = tokens.shape
    halo = SEQ_MAX + PAD
    n_mp = lax.axis_size("mp")
    n_batch = lax.axis_size("batch")
    part = width // n_mp
    ff = w_up.shape[1] * n_mp
    own_start = lax.axis_index("mp") * rows

    packed = jnp.concatenate(
        [w_qkv.reshape(w_qkv.shape[0], -1), w_out.T, w_up, w_down.T], axis=1
    )
    full = lax.all_gather(packed, ("batch", "mp"), axis=0, tiled=False)
    full = full.reshape((n_batch, n_mp) + packed.shape).transpose(0, 2, 1, 3).reshape(width, n_mp, -1)
    cuts = (3 * part, 4 * part, 4 * part + w_up.shape[1])
    full_qkv = full[:, :, : cuts[0]].reshape(width, n_mp, 3, part).transpose(0, 2, 1, 3).reshape(width, 3 * width)
    full_out = full[:, :, cuts[0] : cuts[1]].reshape(width, width)
    full_up = full[:, :, cuts[1] : cuts[2]].reshape(width, ff)
    full_down = full[:, :, cuts[2] :].reshape(width, ff)
    kernel = lax.all_gather(dconv_kernel, "mp", axis=2, tiled=True).transpose(1, 0, 2).reshape(3, 3 * width)

    back = [(i, i + 1) for i in range(n_mp - 1)]
    tok_halo = lax.ppermute(tokens[rows - halo :], "mp", back)
    ext = jnp.concatenate([tok_halo, tokens], axis=0).astype(F32)
    seg_pad = jnp.concatenate([jnp.full((halo,), -1, jnp.int32), seg_ids])
    seg = lax.dynamic_slice_in_dim(seg_pad, own_start, halo + rows, 0)
    same_one = (seg == later(seg, 1)).astype(F32)[:, None]
    same_two = (seg == later(seg, 2)).astype(F32)[:, None]
    slot = own_start + lax.iota(jnp.int32, rows)
    filled = (slot < counts[0]).astype(F32)[:, None]

    scale_one = rms(ext)
    hat_one = ext * scale_one
    normed = (hat_one * gain_attn).astype(BF16)
    projected = nn(normed, full_qkv)
    mixed = (
        kernel[0] * projected
        + kernel[1] * same_one * later(projected, 1)
        + kernel[2] * same_two * later(projected, 2)
    ).astype(BF16)
    queries = mixed[halo:, :width]
    keys = mixed[PAD:, width : 2 * width]
    values = mixed[PAD:, 2 * width :]
    heads, prob = attend(queries, keys, values, seg[PAD:], seg[halo:])
    residual = ext[halo:] + filled * nn(heads, full_out.T if False else full_out.T)
    scale_two = rms(residual)
    hat_two = residual * scale_two
    normed_two = (hat_two * gain_ffn).astype(BF16)
    up = jax.nn.relu(nn(normed_two, full_up))
    hidden = (up * up).astype(BF16)
    layer_out = (residual + filled * nt(hidden, full_down)).astype(BF16)

    grad = grad_out.astype(F32)
    grad_ffn = (filled * grad).astype(BF16)
    grad_up = (nn(grad_ffn, full_down) * 2.0 * up).astype(BF16)
    grad_w_down = tn(grad_ffn, hidden)
    grad_w_up = tn(normed_two, grad_up)
    grad_normed_two = nt(grad_up, full_up)
    grad_resid = grad + rms_back(grad_normed_two, gain_ffn, hat_two, scale_two)
    grad_gain_ffn = jnp.sum(grad_normed_two * hat_two, axis=0)
    grad_attn = (filled * grad_resid).astype(BF16)
    grad_w_out = tn(grad_attn, heads)
    grad_heads = nn(grad_attn, full_out).astype(BF16)
    dq, dk, dv = attend_back(queries, keys, values, grad_heads, prob)
    grad_mixed = jnp.concatenate(
        [
            jnp.pad(dq, ((halo, 0), (0, 0))),
            jnp.pad(dk, ((PAD, 0), (0, 0))),
            jnp.pad(dv, ((PAD, 0), (0, 0))),
        ],
        axis=1,
    )
    one = grad_mixed * same_one
    two = grad_mixed * same_two
    grad_kernel = jnp.stack(
        [
            jnp.sum(grad_mixed * projected, axis=0),
            jnp.sum(one * later(projected, 1), axis=0),
            jnp.sum(two * later(projected, 2), axis=0),
        ]
    )
    grad_proj = (
        kernel[0] * grad_mixed + kernel[1] * sooner(one, 1) + kernel[2] * sooner(two, 2)
    ).astype(BF16)
    grad_w_qkv = tn(normed, grad_proj)
    grad_normed = nt(grad_proj, full_qkv)
    ahead = [(i + 1, i) for i in range(n_mp - 1)]
    passed = lax.ppermute(grad_normed[:halo].astype(BF16), "mp", ahead).astype(F32)
    own_normed = grad_normed[halo:] + jnp.pad(passed, ((rows - halo, 0), (0, 0)))
    grad_tokens = grad_resid + rms_back(own_normed, gain_attn, hat_one[halo:], scale_one[halo:])
    grad_gain_attn = jnp.sum(own_normed * hat_one[halo:], axis=0)

    shard = packed.shape[0]
    grads = jnp.concatenate(
        [
            grad_w_qkv.astype(BF16).reshape(width, 3, n_mp, part).transpose(0, 2, 1, 3).reshape(width, n_mp, -1),
            grad_w_out.astype(BF16).reshape(width, n_mp, -1),
            grad_w_up.astype(BF16).reshape(width, n_mp, -1),
            grad_w_down.astype(BF16).reshape(width, n_mp, -1),
        ],
        axis=2,
    )
    grads = grads.reshape(n_batch, shard, n_mp, -1).transpose(0, 2, 1, 3).reshape(n_batch * n_mp, shard, -1)
    own = lax.psum_scatter(grads, ("batch", "mp"), scatter_dimension=0, tiled=False).astype(F32)
    small = jnp.concatenate(
        [grad_kernel.reshape(3, 3, width).transpose(1, 0, 2).reshape(9, width), grad_gain_attn[None], grad_gain_ffn[None]]
    )
    piece = width // (n_mp * n_batch)
    small = small.reshape(11, n_mp * n_batch, piece).transpose(1, 0, 2)
    small = lax.psum_scatter(small, ("mp", "batch"), scatter_dimension=0, tiled=False)
    return (
        layer_out,
        grad_tokens,
        small[9],
        small[10],
        own[:, : cuts[0]].reshape(shard, 3, part),
        small[:9].reshape(3, 3, piece),
        own[:, cuts[0] : cuts[1]].T,
        own[:, cuts[1] : cuts[2]],
        own[:, cuts[2] :].T,
    )


HALO = SEQ_MAX
BLK = 128
HEADS = ((1, 2, 3, False, False, 0), (1, 2, 3, True, True, 0), (0, 4, 4, True, False, 1))
COLUMNS = 5 * BLK


def blk(index):
    return slice(index * BLK, (index + 1) * BLK)


def half_of(values, upper):
    lane = lax.broadcasted_iota(jnp.int32, values.shape, 1)
    keep = (lane >= HD) if upper else (lane < HD)
    return jnp.where(keep, values, jnp.zeros_like(values))


def rows_loop(total, size, body):
    def one(i, carry):
        body(pl.ds(pl.multiple_of(i * size, size), size))
        return carry

    lax.fori_loop(0, total // size, one, 0)


def parts_loop(count, body):
    def one(i, carry):
        body(i)
        return carry

    lax.fori_loop(0, count, one, 0)


def layer_kernel(
    wa_hbm, wu_hbm, wd_hbm, ext_ref, grad_ref, cols_ref, seg_row_ref, gains_ref, kernel_ref,
    ga_hbm, gu_hbm, gd_hbm, out_ref, resid_grad_ref, own_ref, pass_ref, small_ref, gain_ref,
    wa, wu, wd, ga, gu, gd, normed, proj, mixed, prob, heads, bias, wide, acc, resid, normed_two,
    gffn_t, two_t, normed_t, hidden, upper, lower, in_sems, out_sems,
):
    parts = wa.shape[0]
    rows, width = resid.shape
    span = HALO + rows
    tiles = rows // SEQ_MAX
    tile = SEQ_MAX

    def fetch(hbm, ref, piece, m):
        return pltpu.make_async_copy(hbm.at[m], ref.at[m], in_sems.at[piece, m])

    def put(ref, hbm, piece, m):
        return pltpu.make_async_copy(ref.at[m], hbm.at[m], out_sems.at[piece, m])

    for m in range(parts):
        fetch(wa_hbm, wa, 0, m).start()
    for m in range(parts):
        fetch(wu_hbm, wu, 1, m).start()
        fetch(wd_hbm, wd, 2, m).start()

    gain_one = gains_ref[0:1, :]
    gain_two = gains_ref[1:2, :]

    def norm_one(at):
        values = ext_ref[at, :].astype(F32)
        normed[at, :] = (values * rms(values) * gain_one).astype(BF16)

    rows_loop(span, 128, norm_one)
    for at in range(tiles):
        key = lax.broadcasted_iota(jnp.int32, (2 * tile, tile), 0)
        query = lax.broadcasted_iota(jnp.int32, (2 * tile, tile), 1) + tile
        seg_key = cols_ref[at * tile : (at + 2) * tile, 2:3]
        same = seg_key == seg_row_ref[0:1, at * tile : (at + 1) * tile]
        bias[at] = jnp.where(same & (key <= query), 0.0, MASKED).astype(F32)
    acc[...] = jnp.zeros_like(acc)

    def forward(m):
        fetch(wa_hbm, wa, 0, m).wait()
        wide[...] = nn(normed[...], wa[m, :, BLK:])
        for c in range(5):
            source = wide[:, blk(c)]
            proj[m, :, blk(c)] = source.astype(BF16)
            mixed[m, :, blk(c)] = (
                kernel_ref[m, 0:1, blk(c)] * source
                + kernel_ref[m, 1:2, blk(c)] * (cols_ref[:, 0:1] * pltpu.roll(source, 1, 0))
                + kernel_ref[m, 2:3, blk(c)] * (cols_ref[:, 1:2] * pltpu.roll(source, 2, 0))
            ).astype(BF16)
        for at in range(tiles):
            keys_at = slice(at * tile, (at + 2) * tile)
            query_at = slice(HALO + at * tile, HALO + (at + 1) * tile)
            outs = []
            for h, (qb, kb, vb, qk_upper, v_upper, _) in enumerate(HEADS):
                queries = half_of(mixed[m, query_at, blk(qb)], qk_upper) * jnp.asarray(HD**-0.5, BF16)
                scores = nt(mixed[m, keys_at, blk(kb)], queries) + bias[at]
                expo = jnp.exp(scores - jnp.max(scores, axis=0, keepdims=True))
                share = (expo * (1.0 / jnp.sum(expo, axis=0, keepdims=True))).astype(BF16)
                prob[m, at, h] = share
                outs.append(tn(half_of(mixed[m, keys_at, blk(vb)], v_upper), share))
            own_at = slice(at * tile, (at + 1) * tile)
            heads[m, own_at, blk(0)] = (outs[0] + outs[1]).T.astype(BF16)
            heads[m, own_at, blk(1)] = outs[2].T.astype(BF16)
        acc[...] += nt(heads[m], wa[m, :, : 2 * BLK])

    parts_loop(parts, forward)

    def middle(at):
        values = ext_ref[pl.ds(at.start + HALO, at.size), :].astype(F32)
        filled = cols_ref[pl.ds(at.start + HALO, at.size), 3:4]
        value = values + filled * acc[at, :]
        resid[at, :] = value
        normed_two[at, :] = (value * rms(value) * gain_two).astype(BF16)
        out_ref[at, :] = (filled * grad_ref[at, :].astype(F32)).astype(BF16)

    rows_loop(rows, 128, middle)
    gffn = out_ref
    gffn_t[...] = gffn[...].T
    two_t[...] = normed_two[...].T
    normed_t[...] = normed[...].T
    acc[...] = jnp.zeros_like(acc)
    own_ref[...] = jnp.zeros_like(own_ref)

    def feed(m):
        fetch(wu_hbm, wu, 1, m).wait()
        fetch(wd_hbm, wd, 2, m).wait()
        up = jnp.maximum(nn(normed_two[...], wu[m]), 0.0)
        upper[...] = (2.0 * up).astype(BF16)
        hidden[...] = (up * up).astype(BF16)
        acc[...] += nt(hidden[...], wd[m])
        gd[m] = nn(gffn_t[...], hidden[...]).astype(BF16)
        put(gd, gd_hbm, 2, m).start()
        lower[...] = (nn(gffn[...], wd[m]) * upper[...].astype(F32)).astype(BF16)
        gu[m] = nn(two_t[...], lower[...]).astype(BF16)
        put(gu, gu_hbm, 1, m).start()
        own_ref[...] += nt(lower[...], wu[m])

    parts_loop(parts, feed)

    gain_ref[...] = jnp.zeros_like(gain_ref)

    def turn(at):
        value = resid[at, :]
        filled = cols_ref[pl.ds(at.start + HALO, at.size), 3:4]
        scale = rms(value)
        hat = value * scale
        grad = own_ref[at, :]
        gain_ref[0:1, :] += jnp.sum(grad * hat, axis=0, keepdims=True)
        total = grad_ref[at, :].astype(F32) + rms_back(grad, gain_two, hat, scale)
        resid_grad_ref[at, :] = total
        out_ref[at, :] = (value + filled * acc[at, :]).astype(BF16)
        normed_two[at, :] = (filled * total).astype(BF16)

    rows_loop(rows, 128, turn)
    gattn = normed_two
    two_t[...] = gattn[...].T
    own_ref[...] = jnp.zeros_like(own_ref)
    acc[...] = jnp.zeros_like(acc)

    def backward(m):
        grads = nn(gattn[...], wa[m, :, : 2 * BLK]).astype(BF16)
        hidden[:, : 2 * BLK] = grads
        wide[...] = jnp.zeros_like(wide)
        for at in range(tiles):
            keys_at = slice(at * tile, (at + 2) * tile)
            query_at = slice(HALO + at * tile, HALO + (at + 1) * tile)
            own_at = slice(at * tile, (at + 1) * tile)
            for h, (qb, kb, vb, qk_upper, v_upper, ob) in enumerate(HEADS):
                share = prob[m, at, h]
                grad_head = half_of(hidden[own_at, blk(ob)], v_upper)
                queries = half_of(mixed[m, query_at, blk(qb)], qk_upper) * jnp.asarray(HD**-0.5, BF16)
                grad_prob = nt(mixed[m, keys_at, blk(vb)], grad_head)
                broad = share.astype(F32)
                inner = broad * grad_prob
                grad_scores = (inner - broad * jnp.sum(inner, axis=0, keepdims=True)).astype(BF16)
                wide[keys_at, blk(vb)] += nn(share, grad_head)
                wide[keys_at, blk(kb)] += nn(grad_scores, queries)
                keys = half_of(mixed[m, keys_at, blk(kb)], qk_upper)
                wide[query_at, blk(qb)] += (tn(keys, grad_scores) * HD**-0.5).T
        for c in range(5):
            grad = wide[:, blk(c)]
            one = grad * cols_ref[:, 0:1]
            two = grad * cols_ref[:, 1:2]
            source = proj[m, :, blk(c)].astype(F32)
            small_ref[m, 0:1, blk(c)] = jnp.sum(grad * source, axis=0, keepdims=True)
            small_ref[m, 1:2, blk(c)] = jnp.sum(one * pltpu.roll(source, 1, 0), axis=0, keepdims=True)
            small_ref[m, 2:3, blk(c)] = jnp.sum(two * pltpu.roll(source, 2, 0), axis=0, keepdims=True)
            mixed[m, :, blk(c)] = (
                kernel_ref[m, 0:1, blk(c)] * grad
                + kernel_ref[m, 1:2, blk(c)] * pltpu.roll(one, span - 1, 0)
                + kernel_ref[m, 2:3, blk(c)] * pltpu.roll(two, span - 2, 0)
            ).astype(BF16)
        part = nn(two_t[...], heads[m])
        whole = nn(normed_t[...], mixed[m])
        ga[m, :, blk(0)] = part[:, blk(0)].astype(BF16)
        ga[m, :, blk(1)] = (half_of(part[:, blk(1)], False) + half_of(whole[:, blk(0)], True)).astype(BF16)
        ga[m, :, 2 * BLK :] = whole[:, BLK:].astype(BF16)
        put(ga, ga_hbm, 0, m).start()
        own_ref[...] += nt(mixed[m, HALO:, :], wa[m, :, BLK:])
        acc[:HALO, :] += nt(mixed[m, :HALO, :], wa[m, :, BLK:])

    parts_loop(parts, backward)
    pass_ref[...] = acc[:HALO, :].astype(BF16)
    for m in range(parts):
        put(ga, ga_hbm, 0, m).wait()
        put(gu, gu_hbm, 1, m).wait()
        put(gd, gd_hbm, 2, m).wait()


def layer_call(wa, wu, wd, ext, grad_out, cols, seg_row, gains, kernel):
    parts, width, _ = wa.shape
    rows = grad_out.shape[0]
    span = rows + HALO
    tiles = rows // SEQ_MAX
    vmem = pl.BlockSpec(memory_space=pltpu.VMEM)
    hbm = pl.BlockSpec(memory_space=pl.ANY)
    big = pltpu.VMEM((parts, width, width), BF16)
    return pl.pallas_call(
        layer_kernel,
        in_specs=[hbm] * 3 + [vmem] * 6,
        out_specs=[hbm] * 3 + [vmem] * 6,
        out_shape=[jax.ShapeDtypeStruct((parts, width, width), BF16)] * 3
        + [
            jax.ShapeDtypeStruct((rows, width), BF16),
            jax.ShapeDtypeStruct((rows, width), F32),
            jax.ShapeDtypeStruct((rows, width), F32),
            jax.ShapeDtypeStruct((HALO, width), BF16),
            jax.ShapeDtypeStruct((parts, 3, COLUMNS), F32),
            jax.ShapeDtypeStruct((1, width), F32),
        ],
        scratch_shapes=[
            big, big, big, big, big, big,
            pltpu.VMEM((span, width), BF16),
            pltpu.VMEM((parts, span, COLUMNS), BF16),
            pltpu.VMEM((parts, span, COLUMNS), BF16),
            pltpu.VMEM((parts, tiles, 3, 2 * SEQ_MAX, SEQ_MAX), BF16),
            pltpu.VMEM((parts, rows, 2 * BLK), BF16),
            pltpu.VMEM((tiles, 2 * SEQ_MAX, SEQ_MAX), F32),
            pltpu.VMEM((span, COLUMNS), F32),
            pltpu.VMEM((rows, width), F32),
            pltpu.VMEM((rows, width), F32),
            pltpu.VMEM((rows, width), BF16),
            pltpu.VMEM((width, rows), BF16),
            pltpu.VMEM((width, rows), BF16),
            pltpu.VMEM((width, span), BF16),
            pltpu.VMEM((rows, width), BF16),
            pltpu.VMEM((rows, width), BF16),
            pltpu.VMEM((rows, width), BF16),
            pltpu.SemaphoreType.DMA((3, parts)),
            pltpu.SemaphoreType.DMA((3, parts)),
        ],
        compiler_params=pltpu.CompilerParams(vmem_limit_bytes=67043328),
        name="layer",
    )(wa, wu, wd, ext, grad_out, cols, seg_row, gains, kernel)


def arrange(q, k, v, o):
    cut = lambda a, h: a[..., h * HD : (h + 1) * HD]
    order = [cut(o, 0), cut(o, 1), cut(o, 2), cut(q, 2), cut(q, 0), cut(q, 1)]
    order += [cut(k, 0), cut(k, 1), cut(v, 0), cut(v, 1), cut(v, 2), cut(k, 2)]
    return jnp.concatenate(order, axis=-1)


def disarrange(a):
    cut = lambda i: a[..., i * HD : (i + 1) * HD]
    join = lambda *ids: jnp.concatenate([cut(i) for i in ids], axis=-1)
    return join(4, 5, 3), join(6, 7, 11), join(8, 9, 10), join(0, 1, 2)


def shards(
    tokens, seg_ids, counts, gain_attn, gain_ffn, w_qkv, dconv_kernel, w_out, w_up, w_down, grad_out
):
    rows, width = tokens.shape
    n_mp = lax.axis_size("mp")
    n_batch = lax.axis_size("batch")
    part = width // n_mp
    shard = w_qkv.shape[0]
    fits = (
        rows % SEQ_MAX == 0 and part == 3 * HD and width == 4 * part and shard % 16 == 0
        and w_up.shape[1] == width and seg_ids.shape[0] == n_mp * rows
    )
    if not fits:
        return shards_plain(
            tokens, seg_ids, counts, gain_attn, gain_ffn, w_qkv, dconv_kernel, w_out, w_up, w_down, grad_out
        )
    own_start = lax.axis_index("mp") * rows
    piece_a = arrange(w_qkv[:, 0], w_qkv[:, 1], w_qkv[:, 2], w_out.T)
    pieces = jnp.stack([piece_a, w_up, w_down.T])
    wa, wu, wd = gather(pieces)
    taps = lax.all_gather(dconv_kernel, "mp", axis=0, tiled=False)
    zero = jnp.zeros_like(taps[:, 0])
    kernel = arrange(taps[:, 0], taps[:, 1], taps[:, 2], zero)[..., BLK:]
    back = [(i, i + 1) for i in range(n_mp - 1)]
    ext = jnp.concatenate([lax.ppermute(tokens[rows - HALO :], "mp", back), tokens], axis=0)
    seg_pad = jnp.concatenate([jnp.full((HALO,), -1, jnp.int32), seg_ids])
    seg = lax.dynamic_slice_in_dim(seg_pad, own_start, HALO + rows, 0).astype(F32)
    slot = own_start - HALO + lax.iota(jnp.int32, HALO + rows)
    cols = jnp.stack(
        [
            (seg == later(seg, 1)).astype(F32).at[0].set(0.0),
            (seg == later(seg, 2)).astype(F32).at[:2].set(0.0),
            seg,
            (slot < counts[0]).astype(F32),
        ],
        axis=1,
    )
    gains = jnp.stack([gain_attn, gain_ffn])
    ga, gu, gd, layer_out, resid_grad, own_normed, passed, taps_grad, gain_two = layer_call(
        wa, wu, wd, ext, grad_out, cols, seg[None, HALO:], gains, kernel
    )
    own = scatter(ga, gu, gd)
    ahead = [(i + 1, i) for i in range(n_mp - 1)]
    passed = lax.ppermute(passed, "mp", ahead).astype(F32)
    own_normed = own_normed + jnp.pad(passed, ((rows - HALO, 0), (0, 0)))
    values = tokens.astype(F32)
    scale = rms(values)
    hat = values * scale
    grad_tokens = resid_grad + rms_back(own_normed, gain_attn, hat, scale)
    gain_one = jnp.sum(own_normed * hat, axis=0)
    first, second, third, _ = disarrange(jnp.pad(taps_grad, ((0, 0), (0, 0), (BLK, 0))))
    small = jnp.stack([first, second, third]).transpose(0, 2, 1, 3).reshape(9, width)
    small = jnp.concatenate([small, gain_one[None], gain_two])
    piece = width // (n_mp * n_batch)
    small = small.reshape(11, n_mp * n_batch, piece).transpose(1, 0, 2)
    small = lax.psum_scatter(small, ("mp", "batch"), scatter_dimension=0, tiled=False)
    q, k, v, o = disarrange(own[0])
    return (
        layer_out,
        grad_tokens,
        small[9],
        small[10],
        jnp.stack([q, k, v], axis=1),
        small[:9].reshape(3, 3, piece),
        o.T,
        own[1],
        own[2].T,
    )


def gather(pieces):
    full = lax.all_gather(pieces, ("batch", "mp"), axis=0, tiled=False)
    n_mp = lax.axis_size("mp")
    full = full.reshape((-1, n_mp) + pieces.shape).transpose(2, 1, 0, 3, 4)
    full = full.reshape(3, n_mp, -1, pieces.shape[2])
    return full[0], full[1], full[2]


def scatter(ga, gu, gd):
    n_mp, width, columns = ga.shape
    n_batch = lax.axis_size("batch")
    grads = jnp.stack([ga, gu, gd]).reshape(3, n_mp, n_batch, width // n_batch, columns)
    grads = grads.transpose(2, 1, 0, 3, 4).reshape((-1, 3, width // n_batch, columns))
    return lax.psum_scatter(grads, ("batch", "mp"), scatter_dimension=0, tiled=False).astype(F32)


def solution(mesh):
    in_specs = (
        P(("batch", "mp"), None),
        P("batch"),
        P("batch"),
        P(),
        P(),
        P("batch", None, "mp"),
        P(None, None, "mp"),
        P("mp", "batch"),
        P("batch", "mp"),
        P("mp", "batch"),
        P(("batch", "mp"), None),
    )
    out_specs = (
        P(("batch", "mp"), None),
        P(("batch", "mp"), None),
        P(("mp", "batch")),
        P(("mp", "batch")),
        P("batch", None, "mp"),
        P(None, None, ("mp", "batch")),
        P("mp", "batch"),
        P("batch", "mp"),
        P("mp", "batch"),
    )
    return jax.shard_map(shards, mesh=mesh, in_specs=in_specs, out_specs=out_specs, check_vma=False)
```

```python
import jax
import jax.numpy as jnp
from jax import lax
from jax.experimental import pallas as pl
from jax.experimental.pallas import tpu as pltpu
from jax.sharding import PartitionSpec as P

HD = 64
SEQ_MAX = 256
PAD = 16
EPSILON = 1e-06
MASKED = -1e30
F32 = jnp.float32
BF16 = jnp.bfloat16


def nt(left, right):
    return lax.dot_general(left, right, (((1,), (1,)), ((), ())), preferred_element_type=F32)


def nn(left, right):
    return lax.dot_general(left, right, (((1,), (0,)), ((), ())), preferred_element_type=F32)


def tn(left, right):
    return lax.dot_general(left, right, (((0,), (0,)), ((), ())), preferred_element_type=F32)


def head_mask(values, head):
    lane = lax.broadcasted_iota(jnp.int32, values.shape, 1)
    return jnp.where((lane >= head * HD) & (lane < (head + 1) * HD), values, jnp.zeros_like(values))


def attend_kernel(q_ref, k_ref, v_ref, seg_key_ref, seg_query_ref, out_ref, prob_ref, bias_ref):
    tile = SEQ_MAX
    tiles = q_ref.shape[0] // tile

    @pl.when(pl.program_id(0) == 0)
    def _():
        for at in range(tiles):
            key = lax.broadcasted_iota(jnp.int32, (2 * tile, tile), 0)
            query = lax.broadcasted_iota(jnp.int32, (2 * tile, tile), 1) + tile
            same = seg_key_ref[at * tile : (at + 2) * tile, :] == seg_query_ref[:, at * tile : (at + 1) * tile]
            bias_ref[at] = jnp.where(same & (key <= query), 0.0, MASKED).astype(F32)

    for at in range(tiles):
        keys = k_ref[at * tile : (at + 2) * tile, :]
        values = v_ref[at * tile : (at + 2) * tile, :]
        queries = q_ref[at * tile : (at + 1) * tile, :] * jnp.asarray(HD**-0.5, BF16)
        outs = []
        for head in range(2):
            scores = nt(keys, head_mask(queries, head)) + bias_ref[at]
            expo = jnp.exp(scores - jnp.max(scores, axis=0, keepdims=True))
            prob = (expo * (1.0 / jnp.sum(expo, axis=0, keepdims=True))).astype(BF16)
            prob_ref[0, at, head] = prob
            outs.append(tn(head_mask(values, head), prob))
        out_ref[at * tile : (at + 1) * tile, :] = (outs[0] + outs[1]).T.astype(BF16)


def attend_back_kernel(q_ref, k_ref, v_ref, grad_ref, prob_ref, dq_ref, dk_ref, dv_ref):
    tile = SEQ_MAX
    tiles = q_ref.shape[0] // tile
    dk_ref[...] = jnp.zeros_like(dk_ref)
    dv_ref[...] = jnp.zeros_like(dv_ref)
    for at in range(tiles):
        span = slice(at * tile, (at + 2) * tile)
        keys = k_ref[span, :]
        values = v_ref[span, :]
        queries = q_ref[at * tile : (at + 1) * tile, :] * jnp.asarray(HD**-0.5, BF16)
        grads = grad_ref[at * tile : (at + 1) * tile, :]
        dq = 0.0
        for head in range(2):
            prob = prob_ref[0, at, head]
            grad_head = head_mask(grads, head)
            grad_prob = nt(values, grad_head)
            wide = prob.astype(F32)
            inner = wide * grad_prob
            grad_scores = (inner - wide * jnp.sum(inner, axis=0, keepdims=True)).astype(BF16)
            dv_ref[span, :] += nn(prob, grad_head)
            dk_ref[span, :] += nn(grad_scores, head_mask(queries, head))
            dq = dq + tn(head_mask(keys, head), grad_scores)
        dq_ref[at * tile : (at + 1) * tile, :] = (dq * HD**-0.5).T


def attend(queries, keys, values, seg_key, seg_query):
    rows, width = queries.shape
    span = keys.shape[0]
    tiles = rows // SEQ_MAX
    wide = 2 * HD
    return pl.pallas_call(
        attend_kernel,
        grid=(width // wide,),
        in_specs=[
            pl.BlockSpec((rows, wide), lambda i: (0, i)),
            pl.BlockSpec((span, wide), lambda i: (0, i)),
            pl.BlockSpec((span, wide), lambda i: (0, i)),
            pl.BlockSpec((span, 1), lambda i: (0, 0)),
            pl.BlockSpec((1, rows), lambda i: (0, 0)),
        ],
        out_specs=[
            pl.BlockSpec((rows, wide), lambda i: (0, i)),
            pl.BlockSpec((1, tiles, 2, 2 * SEQ_MAX, SEQ_MAX), lambda i: (i, 0, 0, 0, 0)),
        ],
        out_shape=[
            jax.ShapeDtypeStruct((rows, width), BF16),
            jax.ShapeDtypeStruct((width // wide, tiles, 2, 2 * SEQ_MAX, SEQ_MAX), BF16),
        ],
        scratch_shapes=[pltpu.VMEM((tiles, 2 * SEQ_MAX, SEQ_MAX), F32)],
        name="attend",
    )(queries, keys, values, seg_key[:, None], seg_query[None, :])


def attend_back(queries, keys, values, grads, prob):
    rows, width = queries.shape
    span = keys.shape[0]
    tiles = rows // SEQ_MAX
    wide = 2 * HD
    return pl.pallas_call(
        attend_back_kernel,
        grid=(width // wide,),
        in_specs=[
            pl.BlockSpec((rows, wide), lambda i: (0, i)),
            pl.BlockSpec((span, wide), lambda i: (0, i)),
            pl.BlockSpec((span, wide), lambda i: (0, i)),
            pl.BlockSpec((rows, wide), lambda i: (0, i)),
            pl.BlockSpec((1, tiles, 2, 2 * SEQ_MAX, SEQ_MAX), lambda i: (i, 0, 0, 0, 0)),
        ],
        out_specs=[
            pl.BlockSpec((rows, wide), lambda i: (0, i)),
            pl.BlockSpec((span, wide), lambda i: (0, i)),
            pl.BlockSpec((span, wide), lambda i: (0, i)),
        ],
        out_shape=[
            jax.ShapeDtypeStruct((rows, width), F32),
            jax.ShapeDtypeStruct((span, width), F32),
            jax.ShapeDtypeStruct((span, width), F32),
        ],
        name="attend_back",
    )(queries, keys, values, grads, prob)


def rms(values):
    return lax.rsqrt(jnp.mean(values * values, axis=-1, keepdims=True) + EPSILON)


def rms_back(grad, gain, hat, scale):
    scaled = grad * gain
    return scale * (scaled - hat * jnp.mean(scaled * hat, axis=-1, keepdims=True))


def later(values, by):
    return jnp.concatenate([jnp.zeros((by,) + values.shape[1:], values.dtype), values[:-by]], axis=0)


def sooner(values, by):
    return jnp.concatenate([values[by:], jnp.zeros((by,) + values.shape[1:], values.dtype)], axis=0)


def shards_plain(
    tokens, seg_ids, counts, gain_attn, gain_ffn, w_qkv, dconv_kernel, w_out, w_up, w_down, grad_out
):
    rows, width = tokens.shape
    halo = SEQ_MAX + PAD
    n_mp = lax.axis_size("mp")
    n_batch = lax.axis_size("batch")
    part = width // n_mp
    ff = w_up.shape[1] * n_mp
    own_start = lax.axis_index("mp") * rows

    packed = jnp.concatenate(
        [w_qkv.reshape(w_qkv.shape[0], -1), w_out.T, w_up, w_down.T], axis=1
    )
    full = lax.all_gather(packed, ("batch", "mp"), axis=0, tiled=False)
    full = full.reshape((n_batch, n_mp) + packed.shape).transpose(0, 2, 1, 3).reshape(width, n_mp, -1)
    cuts = (3 * part, 4 * part, 4 * part + w_up.shape[1])
    full_qkv = full[:, :, : cuts[0]].reshape(width, n_mp, 3, part).transpose(0, 2, 1, 3).reshape(width, 3 * width)
    full_out = full[:, :, cuts[0] : cuts[1]].reshape(width, width)
    full_up = full[:, :, cuts[1] : cuts[2]].reshape(width, ff)
    full_down = full[:, :, cuts[2] :].reshape(width, ff)
    kernel = lax.all_gather(dconv_kernel, "mp", axis=2, tiled=True).transpose(1, 0, 2).reshape(3, 3 * width)

    back = [(i, i + 1) for i in range(n_mp - 1)]
    tok_halo = lax.ppermute(tokens[rows - halo :], "mp", back)
    ext = jnp.concatenate([tok_halo, tokens], axis=0).astype(F32)
    seg_pad = jnp.concatenate([jnp.full((halo,), -1, jnp.int32), seg_ids])
    seg = lax.dynamic_slice_in_dim(seg_pad, own_start, halo + rows, 0)
    same_one = (seg == later(seg, 1)).astype(F32)[:, None]
    same_two = (seg == later(seg, 2)).astype(F32)[:, None]
    slot = own_start + lax.iota(jnp.int32, rows)
    filled = (slot < counts[0]).astype(F32)[:, None]

    scale_one = rms(ext)
    hat_one = ext * scale_one
    normed = (hat_one * gain_attn).astype(BF16)
    projected = nn(normed, full_qkv)
    mixed = (
        kernel[0] * projected
        + kernel[1] * same_one * later(projected, 1)
        + kernel[2] * same_two * later(projected, 2)
    ).astype(BF16)
    queries = mixed[halo:, :width]
    keys = mixed[PAD:, width : 2 * width]
    values = mixed[PAD:, 2 * width :]
    heads, prob = attend(queries, keys, values, seg[PAD:], seg[halo:])
    residual = ext[halo:] + filled * nn(heads, full_out.T if False else full_out.T)
    scale_two = rms(residual)
    hat_two = residual * scale_two
    normed_two = (hat_two * gain_ffn).astype(BF16)
    up = jax.nn.relu(nn(normed_two, full_up))
    hidden = (up * up).astype(BF16)
    layer_out = (residual + filled * nt(hidden, full_down)).astype(BF16)

    grad = grad_out.astype(F32)
    grad_ffn = (filled * grad).astype(BF16)
    grad_up = (nn(grad_ffn, full_down) * 2.0 * up).astype(BF16)
    grad_w_down = tn(grad_ffn, hidden)
    grad_w_up = tn(normed_two, grad_up)
    grad_normed_two = nt(grad_up, full_up)
    grad_resid = grad + rms_back(grad_normed_two, gain_ffn, hat_two, scale_two)
    grad_gain_ffn = jnp.sum(grad_normed_two * hat_two, axis=0)
    grad_attn = (filled * grad_resid).astype(BF16)
    grad_w_out = tn(grad_attn, heads)
    grad_heads = nn(grad_attn, full_out).astype(BF16)
    dq, dk, dv = attend_back(queries, keys, values, grad_heads, prob)
    grad_mixed = jnp.concatenate(
        [
            jnp.pad(dq, ((halo, 0), (0, 0))),
            jnp.pad(dk, ((PAD, 0), (0, 0))),
            jnp.pad(dv, ((PAD, 0), (0, 0))),
        ],
        axis=1,
    )
    one = grad_mixed * same_one
    two = grad_mixed * same_two
    grad_kernel = jnp.stack(
        [
            jnp.sum(grad_mixed * projected, axis=0),
            jnp.sum(one * later(projected, 1), axis=0),
            jnp.sum(two * later(projected, 2), axis=0),
        ]
    )
    grad_proj = (
        kernel[0] * grad_mixed + kernel[1] * sooner(one, 1) + kernel[2] * sooner(two, 2)
    ).astype(BF16)
    grad_w_qkv = tn(normed, grad_proj)
    grad_normed = nt(grad_proj, full_qkv)
    ahead = [(i + 1, i) for i in range(n_mp - 1)]
    passed = lax.ppermute(grad_normed[:halo].astype(BF16), "mp", ahead).astype(F32)
    own_normed = grad_normed[halo:] + jnp.pad(passed, ((rows - halo, 0), (0, 0)))
    grad_tokens = grad_resid + rms_back(own_normed, gain_attn, hat_one[halo:], scale_one[halo:])
    grad_gain_attn = jnp.sum(own_normed * hat_one[halo:], axis=0)

    shard = packed.shape[0]
    grads = jnp.concatenate(
        [
            grad_w_qkv.astype(BF16).reshape(width, 3, n_mp, part).transpose(0, 2, 1, 3).reshape(width, n_mp, -1),
            grad_w_out.astype(BF16).reshape(width, n_mp, -1),
            grad_w_up.astype(BF16).reshape(width, n_mp, -1),
            grad_w_down.astype(BF16).reshape(width, n_mp, -1),
        ],
        axis=2,
    )
    grads = grads.reshape(n_batch, shard, n_mp, -1).transpose(0, 2, 1, 3).reshape(n_batch * n_mp, shard, -1)
    own = lax.psum_scatter(grads, ("batch", "mp"), scatter_dimension=0, tiled=False).astype(F32)
    small = jnp.concatenate(
        [grad_kernel.reshape(3, 3, width).transpose(1, 0, 2).reshape(9, width), grad_gain_attn[None], grad_gain_ffn[None]]
    )
    piece = width // (n_mp * n_batch)
    small = small.reshape(11, n_mp * n_batch, piece).transpose(1, 0, 2)
    small = lax.psum_scatter(small, ("mp", "batch"), scatter_dimension=0, tiled=False)
    return (
        layer_out,
        grad_tokens,
        small[9],
        small[10],
        own[:, : cuts[0]].reshape(shard, 3, part),
        small[:9].reshape(3, 3, piece),
        own[:, cuts[0] : cuts[1]].T,
        own[:, cuts[1] : cuts[2]],
        own[:, cuts[2] :].T,
    )


HALO = SEQ_MAX
BLK = 128
HEADS = ((1, 2, 3, False, False, 0), (1, 2, 3, True, True, 0), (0, 4, 4, True, False, 1))
COLUMNS = 5 * BLK


def blk(index):
    return slice(index * BLK, (index + 1) * BLK)


def half_of(values, upper):
    lane = lax.broadcasted_iota(jnp.int32, values.shape, 1)
    keep = (lane >= HD) if upper else (lane < HD)
    return jnp.where(keep, values, jnp.zeros_like(values))


def rows_loop(total, size, body):
    def one(i, carry):
        body(pl.ds(pl.multiple_of(i * size, size), size))
        return carry

    lax.fori_loop(0, total // size, one, 0)


def parts_loop(count, body):
    def one(i, carry):
        body(i)
        return carry

    lax.fori_loop(0, count, one, 0)


MESH = pl.DeviceIdType.MESH


def meet_all():
    barrier = pltpu.get_barrier_semaphore()
    others = 0
    for axis in ("batch", "mp"):
        size = lax.axis_size(axis)
        for by in range(1, size):
            other = lax.rem(lax.axis_index(axis) + by, size)
            pl.semaphore_signal(barrier, inc=1, device_id={axis: other}, device_id_type=MESH)
        others += size - 1
    pl.semaphore_wait(barrier, others)


class Place:
    def __init__(self):
        self.b = lax.axis_index("batch")
        self.m = lax.axis_index("mp")
        self.zs = lax.axis_size("batch") // 2
        self.z = self.b // 2
        self.y = lax.rem(self.b, 2)

    def behind(self, k):
        return lax.rem(self.z + self.zs - k, self.zs) * 2

    def ahead(self, k):
        return lax.rem(self.z + k, self.zs) * 2

    def flip_x(self):
        return lax.rem(self.m + 2, 4)

    def flip_core(self, m):
        return m + 1 - 2 * lax.rem(m, 2)


class Gather:
    def __init__(self, pieces, w, send_sems, recv_sems, own_sems):
        self.pieces, self.w, self.send, self.recv, self.own = pieces, w, send_sems, recv_sems, own_sems
        self.at = Place()
        self.shard = pieces.shape[1]
        self.half = self.shard // 2

    def spot(self, p, c, k, j, core=False):
        at = self.at
        cross_y = j in ((1, 3) if c == 0 else (2, 3))
        cross_x = j in ((2, 3) if c == 0 else (1, 3))
        b = at.behind(k) + (1 - at.y if cross_y else at.y)
        m = at.flip_x() if cross_x else at.m
        m = at.flip_core(m) if core else m
        first = pl.multiple_of(b * self.shard + c * self.half, 16)
        return self.w.at[p, m, pl.ds(first, self.half), :]

    def copy(self, p, c, k, j, number, target, core=False):
        own = self.pieces.at[p, c * self.half : (c + 1) * self.half, :]
        return pltpu.make_async_remote_copy(
            own if (k, j) == (0, 0) else self.spot(p, c, k, j),
            self.spot(p, c, k, j),
            self.send.at[p, c, number],
            self.recv.at[p, c, number],
            device_id=target,
            device_id_type=MESH,
        )

    def to(self, axis):
        at = self.at
        return {"batch": at.z * 2 + 1 - at.y} if axis == "y" else {"mp": at.flip_x()}

    def hops(self, p, c, k, j):
        zs = self.at.zs
        axes = ("y", "x") if c == 0 else ("x", "y")
        out = []
        if (k, j) == (0, 0):
            for by in range(1, zs):
                out.append(self.copy(p, c, k, j, by - 1, {"batch": self.at.ahead(by) + self.at.y}))
        if j == 0:
            out.append(self.copy(p, c, k, j, zs - 1 + k, self.to(axes[0])))
        if j in (0, 1):
            out.append(self.copy(p, c, k, j, 2 * zs - 1 + 2 * k + j, self.to(axes[1])))
        out.append(self.copy(p, c, k, j, 4 * zs - 1 + 4 * k + j, {"mp": self.at.flip_core(self.at.m)}))
        return out

    def arrived(self, p, c, k, j):
        zs = self.at.zs
        number = (k - 1, zs - 1 + k, 2 * zs - 1 + 2 * k, 2 * zs + 2 * k)[j]
        self.wait(p, c, number, self.spot(p, c, k, j))

    def wait(self, p, c, number, ref):
        pltpu.make_async_copy(ref, ref, self.recv.at[p, c, number]).wait()

    def begin(self, p):
        own = self.w.at[p, self.at.m, pl.ds(pl.multiple_of(self.at.b * self.shard, 16), self.shard), :]
        pltpu.make_async_copy(self.pieces.at[p], own, self.own.at[p]).start()
        for c in range(2):
            for hop in self.hops(p, c, 0, 0):
                hop.start()

    def relay(self, p, c, k, j):
        self.arrived(p, c, k, j)
        for hop in self.hops(p, c, k, j):
            hop.start()

    def relay_all(self, p):
        for j in range(4):
            for k in range(self.at.zs):
                for c in range(2):
                    if (k, j) != (0, 0):
                        self.relay(p, c, k, j)

    def finish(self, p):
        own = self.w.at[p, self.at.m, pl.ds(pl.multiple_of(self.at.b * self.shard, 16), self.shard), :]
        pltpu.make_async_copy(self.pieces.at[p], own, self.own.at[p]).wait()
        for k in range(self.at.zs):
            for j in range(4):
                for c in range(2):
                    self.wait(p, c, 4 * self.at.zs - 1 + 4 * k + j, self.spot(p, c, k, j, core=True))

    def drain(self):
        for p in range(3):
            for c in range(2):
                for k in range(self.at.zs):
                    for j in range(4):
                        for hop in self.hops(p, c, k, j):
                            hop.wait_send()


def layer_kernel(
    pieces_ref, tok_ref, grad_ref, cols_ref, seg_row_ref, gains_ref, kernel_ref,
    g_hbm, out_ref, resid_grad_ref, own_ref, pass_ref, small_ref,
    w, g, ext_ref, normed, proj, mixed, prob, heads, bias, wide, acc, resid, normed_two,
    gffn_t, two_t, normed_t, hidden, upper, lower, send_sems, recv_sems, own_sems, halo_sems, out_sems,
):
    parts = w.shape[1]
    rows, width = resid.shape
    span = HALO + rows
    tiles = rows // SEQ_MAX
    tile = SEQ_MAX

    wa, wu, wd = w.at[0], w.at[1], w.at[2]
    ga, gu, gd = g.at[0], g.at[1], g.at[2]
    pull = Gather(pieces_ref, w, send_sems, recv_sems, own_sems)

    def put(piece, m):
        return pltpu.make_async_copy(g.at[piece, m], g_hbm.at[piece, m], out_sems.at[piece, m])

    meet_all()
    pass_on = pltpu.make_async_remote_copy(
        tok_ref.at[rows - HALO :],
        ext_ref.at[:HALO],
        halo_sems.at[0],
        halo_sems.at[1],
        device_id={"mp": lax.rem(lax.axis_index("mp") + 1, parts)},
        device_id_type=MESH,
    )
    pass_on.start()
    for p in range(3):
        pull.begin(p)
    ext_ref[HALO:, :] = tok_ref[...]

    gain_one = gains_ref[0:1, :]
    gain_two = gains_ref[1:2, :]

    def norm_one(at):
        values = ext_ref[at, :].astype(F32)
        normed[at, :] = (values * rms(values) * gain_one).astype(BF16)

    pass_on.wait()
    rows_loop(span, 128, norm_one)
    for at in range(tiles):
        key = lax.broadcasted_iota(jnp.int32, (2 * tile, tile), 0)
        query = lax.broadcasted_iota(jnp.int32, (2 * tile, tile), 1) + tile
        seg_key = cols_ref[at * tile : (at + 2) * tile, 2:3]
        same = seg_key == seg_row_ref[0:1, at * tile : (at + 1) * tile]
        bias[at] = jnp.where(same & (key <= query), 0.0, MASKED).astype(F32)
    acc[...] = jnp.zeros_like(acc)

    def forward(m):
        wide[...] = nn(normed[...], wa[m, :, BLK:])
        for c in range(5):
            source = wide[:, blk(c)]
            proj[m, :, blk(c)] = source.astype(BF16)
            mixed[m, :, blk(c)] = (
                kernel_ref[m, 0:1, blk(c)] * source
                + kernel_ref[m, 1:2, blk(c)] * (cols_ref[:, 0:1] * pltpu.roll(source, 1, 0))
                + kernel_ref[m, 2:3, blk(c)] * (cols_ref[:, 1:2] * pltpu.roll(source, 2, 0))
            ).astype(BF16)
        for at in range(tiles):
            keys_at = slice(at * tile, (at + 2) * tile)
            query_at = slice(HALO + at * tile, HALO + (at + 1) * tile)
            outs = []
            for h, (qb, kb, vb, qk_upper, v_upper, _) in enumerate(HEADS):
                queries = half_of(mixed[m, query_at, blk(qb)], qk_upper) * jnp.asarray(HD**-0.5, BF16)
                scores = nt(mixed[m, keys_at, blk(kb)], queries) + bias[at]
                expo = jnp.exp(scores - jnp.max(scores, axis=0, keepdims=True))
                share = (expo * (1.0 / jnp.sum(expo, axis=0, keepdims=True))).astype(BF16)
                prob[m, at, h] = share
                outs.append(tn(half_of(mixed[m, keys_at, blk(vb)], v_upper), share))
            own_at = slice(at * tile, (at + 1) * tile)
            heads[m, own_at, blk(0)] = (outs[0] + outs[1]).T.astype(BF16)
            heads[m, own_at, blk(1)] = outs[2].T.astype(BF16)
        acc[...] += nt(heads[m], wa[m, :, : 2 * BLK])

    for p in range(3):
        pull.relay_all(p)
    for p in range(3):
        pull.finish(p)
    parts_loop(parts, forward)

    def middle(at):
        values = ext_ref[pl.ds(at.start + HALO, at.size), :].astype(F32)
        filled = cols_ref[pl.ds(at.start + HALO, at.size), 3:4]
        value = values + filled * acc[at, :]
        resid[at, :] = value
        normed_two[at, :] = (value * rms(value) * gain_two).astype(BF16)
        out_ref[at, :] = (filled * grad_ref[at, :].astype(F32)).astype(BF16)

    rows_loop(rows, 128, middle)
    gffn = out_ref
    gffn_t[...] = gffn[...].T
    two_t[...] = normed_two[...].T
    normed_t[...] = normed[...].T
    acc[...] = jnp.zeros_like(acc)
    own_ref[...] = jnp.zeros_like(own_ref)

    def feed(m):
        up = jnp.maximum(nn(normed_two[...], wu[m]), 0.0)
        upper[...] = (2.0 * up).astype(BF16)
        hidden[...] = (up * up).astype(BF16)
        acc[...] += nt(hidden[...], wd[m])
        gd[m] = nn(gffn_t[...], hidden[...]).astype(BF16)
        put(2, m).start()
        lower[...] = (nn(gffn[...], wd[m]) * upper[...].astype(F32)).astype(BF16)
        gu[m] = nn(two_t[...], lower[...]).astype(BF16)
        put(1, m).start()
        own_ref[...] += nt(lower[...], wu[m])

    parts_loop(parts, feed)

    small_ref[...] = jnp.zeros_like(small_ref)

    def turn(at):
        value = resid[at, :]
        filled = cols_ref[pl.ds(at.start + HALO, at.size), 3:4]
        scale = rms(value)
        hat = value * scale
        grad = own_ref[at, :]
        small_ref[0, 4:5, :] += jnp.sum(grad * hat, axis=0, keepdims=True)
        total = grad_ref[at, :].astype(F32) + rms_back(grad, gain_two, hat, scale)
        resid_grad_ref[at, :] = total
        out_ref[at, :] = (value + filled * acc[at, :]).astype(BF16)
        normed_two[at, :] = (filled * total).astype(BF16)

    rows_loop(rows, 128, turn)
    gattn = normed_two
    two_t[...] = gattn[...].T
    own_ref[...] = jnp.zeros_like(own_ref)
    acc[...] = jnp.zeros_like(acc)

    def backward(m):
        grads = nn(gattn[...], wa[m, :, : 2 * BLK]).astype(BF16)
        hidden[:, : 2 * BLK] = grads
        wide[...] = jnp.zeros_like(wide)
        for at in range(tiles):
            keys_at = slice(at * tile, (at + 2) * tile)
            query_at = slice(HALO + at * tile, HALO + (at + 1) * tile)
            own_at = slice(at * tile, (at + 1) * tile)
            for h, (qb, kb, vb, qk_upper, v_upper, ob) in enumerate(HEADS):
                share = prob[m, at, h]
                grad_head = half_of(hidden[own_at, blk(ob)], v_upper)
                queries = half_of(mixed[m, query_at, blk(qb)], qk_upper) * jnp.asarray(HD**-0.5, BF16)
                grad_prob = nt(mixed[m, keys_at, blk(vb)], grad_head)
                broad = share.astype(F32)
                inner = broad * grad_prob
                grad_scores = (inner - broad * jnp.sum(inner, axis=0, keepdims=True)).astype(BF16)
                wide[keys_at, blk(vb)] += nn(share, grad_head)
                wide[keys_at, blk(kb)] += nn(grad_scores, queries)
                keys = half_of(mixed[m, keys_at, blk(kb)], qk_upper)
                wide[query_at, blk(qb)] += (tn(keys, grad_scores) * HD**-0.5).T
        for c in range(5):
            grad = wide[:, blk(c)]
            one = grad * cols_ref[:, 0:1]
            two = grad * cols_ref[:, 1:2]
            source = proj[m, :, blk(c)].astype(F32)
            small_ref[m, 0:1, blk(c + 1)] = jnp.sum(grad * source, axis=0, keepdims=True)
            small_ref[m, 1:2, blk(c + 1)] = jnp.sum(one * pltpu.roll(source, 1, 0), axis=0, keepdims=True)
            small_ref[m, 2:3, blk(c + 1)] = jnp.sum(two * pltpu.roll(source, 2, 0), axis=0, keepdims=True)
            mixed[m, :, blk(c)] = (
                kernel_ref[m, 0:1, blk(c)] * grad
                + kernel_ref[m, 1:2, blk(c)] * pltpu.roll(one, span - 1, 0)
                + kernel_ref[m, 2:3, blk(c)] * pltpu.roll(two, span - 2, 0)
            ).astype(BF16)
        part = nn(two_t[...], heads[m])
        whole = nn(normed_t[...], mixed[m])
        ga[m, :, blk(0)] = part[:, blk(0)].astype(BF16)
        ga[m, :, blk(1)] = (half_of(part[:, blk(1)], False) + half_of(whole[:, blk(0)], True)).astype(BF16)
        ga[m, :, 2 * BLK :] = whole[:, BLK:].astype(BF16)
        put(0, m).start()
        own_ref[...] += nt(mixed[m, HALO:, :], wa[m, :, BLK:])
        acc[:HALO, :] += nt(mixed[m, :HALO, :], wa[m, :, BLK:])

    parts_loop(parts, backward)
    pass_ref[...] = acc[:HALO, :].astype(BF16)

    def gain_rows(at, grad):
        values = ext_ref[at, :].astype(F32)
        small_ref[0, 3:4, :] += jnp.sum(grad * (values * rms(values)), axis=0, keepdims=True)

    rows_loop(HALO, 128, lambda at: gain_rows(at, acc[at, :]))
    rows_loop(rows, 128, lambda at: gain_rows(pl.ds(at.start + HALO, at.size), own_ref[at, :]))
    for m in range(1, parts):
        small_ref[m, 3:5, :] = small_ref[0, 3:5, :]
    pull.drain()
    for m in range(parts):
        put(0, m).wait()
        put(1, m).wait()
        put(2, m).wait()


def layer_call(pieces, tokens, grad_out, cols, seg_row, gains, kernel):
    parts = lax.axis_size("mp")
    rows, width = grad_out.shape
    span = rows + HALO
    tiles = rows // SEQ_MAX
    copies = 8 * (lax.axis_size("batch") // 2) - 1
    vmem = pl.BlockSpec(memory_space=pltpu.VMEM)
    hbm = pl.BlockSpec(memory_space=pl.ANY)
    big = pltpu.VMEM((3, parts, width, width), BF16)
    return pl.pallas_call(
        layer_kernel,
        in_specs=[vmem] * 7,
        out_specs=[hbm] + [vmem] * 5,
        out_shape=[
            jax.ShapeDtypeStruct((3, parts, width, width), BF16),
            jax.ShapeDtypeStruct((rows, width), BF16),
            jax.ShapeDtypeStruct((rows, width), F32),
            jax.ShapeDtypeStruct((rows, width), F32),
            jax.ShapeDtypeStruct((HALO, width), BF16),
            jax.ShapeDtypeStruct((parts, 8, width), F32),
        ],
        scratch_shapes=[
            big, big,
            pltpu.VMEM((span, width), BF16),
            pltpu.VMEM((span, width), BF16),
            pltpu.VMEM((parts, span, COLUMNS), BF16),
            pltpu.VMEM((parts, span, COLUMNS), BF16),
            pltpu.VMEM((parts, tiles, 3, 2 * SEQ_MAX, SEQ_MAX), BF16),
            pltpu.VMEM((parts, rows, 2 * BLK), BF16),
            pltpu.VMEM((tiles, 2 * SEQ_MAX, SEQ_MAX), F32),
            pltpu.VMEM((span, COLUMNS), F32),
            pltpu.VMEM((rows, width), F32),
            pltpu.VMEM((rows, width), F32),
            pltpu.VMEM((rows, width), BF16),
            pltpu.VMEM((width, rows), BF16),
            pltpu.VMEM((width, rows), BF16),
            pltpu.VMEM((width, span), BF16),
            pltpu.VMEM((rows, width), BF16),
            pltpu.VMEM((rows, width), BF16),
            pltpu.VMEM((rows, width), BF16),
            pltpu.SemaphoreType.DMA((3, 2, copies)),
            pltpu.SemaphoreType.DMA((3, 2, copies)),
            pltpu.SemaphoreType.DMA((3,)),
            pltpu.SemaphoreType.DMA((2,)),
            pltpu.SemaphoreType.DMA((3, parts)),
        ],
        compiler_params=pltpu.CompilerParams(
            vmem_limit_bytes=67043328, collective_id=0, has_side_effects=True
        ),
        name="layer",
    )(pieces, tokens, grad_out, cols, seg_row, gains, kernel)


class Reduce:
    def __init__(self, g_hbm, g, one, two, three, four, sems):
        self.g_hbm, self.g, self.one, self.two, self.three, self.four, self.sems = g_hbm, g, one, two, three, four, sems
        self.at = Place()
        self.x = self.at.m // 2
        self.core = lax.rem(self.at.m, 2)
        self.half = g.shape[4] // 2

    def z(self, k):
        return self.at.ahead(k) // 2

    def lanes(self, c):
        return slice(c * self.half, (c + 1) * self.half)

    def remote(self, source, target, number, device):
        return pltpu.make_async_remote_copy(
            source,
            target,
            self.sems.at[(0,) + number],
            self.sems.at[(1,) + number],
            device_id=device,
            device_id_type=MESH,
        )

    def load(self, p, k):
        z = self.z(k)
        return pltpu.make_async_copy(self.g_hbm.at[p, :, self.core, z], self.g.at[p, :, z], self.sems.at[0, p, k, 7])

    def first(self, p, k):
        other = {"mp": self.at.flip_core(self.at.m)}
        return self.remote(self.g_hbm.at[p, :, 1 - self.core, self.z(k)], self.one.at[p, k], (p, k, 0), other)

    def second(self, p, k, c):
        z, at = self.z(k), self.at
        if c == 0:
            source, device = self.g.at[p, 1 - self.x, z, :, self.lanes(0), :], {"mp": at.flip_x()}
        else:
            source = self.g.at[p, :, z, 1 - at.y, self.lanes(1), :]
            device = {"batch": at.z * 2 + 1 - at.y}
        return self.remote(source, self.two.at[p, k, c], (p, k, 1 + c), device)

    def third(self, p, k, c):
        z, at = self.z(k), self.at
        if c == 0:
            source, device = self.g.at[p, self.x, z, 1 - at.y, self.lanes(0), :], {"batch": at.z * 2 + 1 - at.y}
        else:
            source, device = self.g.at[p, 1 - self.x, z, at.y, self.lanes(1), :], {"mp": at.flip_x()}
        return self.remote(source, self.three.at[p, k, c], (p, k, 3 + c), device)

    def fourth(self, p, k, c):
        at = self.at
        source = self.g.at[p, self.x, self.z(k), at.y, self.lanes(c), :]
        return self.remote(source, self.four.at[p, k - 1, c], (p, k, 5 + c), {"batch": at.ahead(k) + at.y})

    def start(self, p, k):
        self.load(p, k).start()
        self.first(p, k).start()

    def step_one(self, p, k):
        z = self.z(k)
        self.load(p, k).wait()
        self.first(p, k).wait_recv()
        for x in range(2):
            self.g[p, x, z] += self.one[p, k, x]
        for c in range(2):
            self.second(p, k, c).start()

    def step_two(self, p, k):
        z, at = self.z(k), self.at
        self.second(p, k, 0).wait_recv()
        for y in range(2):
            self.g[p, self.x, z, y, self.lanes(0), :] += self.two[p, k, 0, y]
        self.third(p, k, 0).start()
        self.second(p, k, 1).wait_recv()
        for x in range(2):
            self.g[p, x, z, at.y, self.lanes(1), :] += self.two[p, k, 1, x]
        self.third(p, k, 1).start()

    def step_three(self, p, k):
        z, at = self.z(k), self.at
        for c in range(2):
            self.third(p, k, c).wait_recv()
            self.g[p, self.x, z, at.y, self.lanes(c), :] += self.three[p, k, c]
            if k:
                self.fourth(p, k, c).start()

    def step_four(self, p, out):
        for c in range(2):
            total = self.g[p, self.x, self.at.z, self.at.y, self.lanes(c), :].astype(F32)
            for k in range(1, self.at.zs):
                self.fourth(p, k, c).wait_recv()
                total = total + self.four[p, k - 1, c].astype(F32)
            out[p, self.lanes(c), :] = total

    def drain(self, p, k):
        self.first(p, k).wait_send()
        for c in range(2):
            self.second(p, k, c).wait_send()
            self.third(p, k, c).wait_send()
            if k:
                self.fourth(p, k, c).wait_send()


class Small:
    def __init__(self, source, one, two, three, sums, sems):
        self.source, self.one, self.two, self.three, self.sums, self.sems = source, one, two, three, sums, sems
        self.at = Place()
        self.x = self.at.m // 2
        self.core = lax.rem(self.at.m, 2)
        self.count = lax.axis_size("batch")

    def remote(self, source, target, number, device):
        return pltpu.make_async_remote_copy(
            source, target, self.sems.at[0, number], self.sems.at[1, number], device_id=device, device_id_type=MESH
        )

    def core_copy(self, x):
        device = {"mp": self.at.flip_core(self.at.m)}
        return self.remote(self.source.at[x * 2 + 1 - self.core], self.one.at[x], x, device)

    def x_copy(self):
        return self.remote(self.sums.at[1 - self.x], self.two, 2, {"mp": self.at.flip_x()})

    def far_copy(self, by):
        other = lax.rem(self.at.b + by, self.count)
        return self.remote(self.sums.at[self.x], self.three.at[by - 1], 2 + by, {"batch": other})

    def begin(self):
        for x in range(2):
            self.core_copy(x).start()

    def middle(self):
        for x in range(2):
            self.core_copy(x).wait_recv()
            self.sums[x] = self.source[x * 2 + self.core] + self.one[x]
        self.x_copy().start()

    def later(self):
        self.x_copy().wait_recv()
        self.sums[self.x] += self.two[...]
        for by in range(1, self.count):
            self.far_copy(by).start()

    def finish(self, out):
        total = self.sums[self.x]
        for by in range(1, self.count):
            self.far_copy(by).wait_recv()
            total = total + self.three[by - 1]
        out[...] = total
        for x in range(2):
            self.core_copy(x).wait_send()
        self.x_copy().wait_send()
        for by in range(1, self.count):
            self.far_copy(by).wait_send()


def reduce_kernel(
    g_hbm, small_ref, pass_ref, resid_grad_ref, own_ref, tok_ref, gains_ref, own_out, tokens_out, small_out,
    g, one, two, three, four, passed, s_sums, s_one, s_two, s_three, sems, small_sems, pass_sems,
):
    parts = lax.axis_size("mp")
    rows = tok_ref.shape[0]
    meet_all()
    push = Reduce(g_hbm, g, one, two, three, four, sems)
    small = Small(small_ref, s_one, s_two, s_three, s_sums, small_sems)
    me = lax.axis_index("mp")
    pass_on = pltpu.make_async_remote_copy(
        pass_ref,
        passed,
        pass_sems.at[0],
        pass_sems.at[1],
        device_id={"mp": lax.rem(me + parts - 1, parts)},
        device_id_type=MESH,
    )
    zs = push.at.zs
    chunks = [(p, k) for p in (2, 1, 0) for k in [*range(1, zs), 0]]
    for chunk in chunks[:4]:
        push.start(*chunk)
    small.begin()
    pass_on.start()
    for chunk in chunks[4:]:
        push.start(*chunk)

    def last(at, extra):
        values = tok_ref[at, :].astype(F32)
        scale = rms(values)
        tokens_out[at, :] = resid_grad_ref[at, :] + rms_back(
            own_ref[at, :] + extra, gains_ref[0:1, :], values * scale, scale
        )

    def end_rows(at):
        keep = jnp.where(me < parts - 1, 1.0, 0.0)
        last(pl.ds(at.start + rows - HALO, at.size), passed[at, :].astype(F32) * keep)

    for n in range(len(chunks) + 4):
        if n < len(chunks):
            push.step_one(*chunks[n])
        if 0 <= n - 2 < len(chunks):
            push.step_two(*chunks[n - 2])
        if 0 <= n - 4 < len(chunks):
            p, k = chunks[n - 4]
            push.step_three(p, k)
            if k == 0 and p != 2:
                push.step_four(p + 1, own_out)
        if n == 1:
            small.middle()
        if n == 3:
            small.later()
            pass_on.wait()
            rows_loop(rows - HALO, 128, lambda at: last(at, 0.0))
            rows_loop(HALO, 128, end_rows)
    push.step_four(0, own_out)
    small.finish(small_out)
    for chunk in chunks:
        push.drain(*chunk)


def reduce_call(g_hbm, small, passed, resid_grad, own, tokens, gains):
    rows, width = tokens.shape
    zs = lax.axis_size("batch") // 2
    shard = width // (2 * zs)
    half = shard // 2
    vmem = pl.BlockSpec(memory_space=pltpu.VMEM)
    return pl.pallas_call(
        reduce_kernel,
        in_specs=[pl.BlockSpec(memory_space=pl.ANY)] + [vmem] * 6,
        out_specs=[vmem] * 3,
        out_shape=[
            jax.ShapeDtypeStruct((3, shard, width), F32),
            jax.ShapeDtypeStruct((rows, width), F32),
            jax.ShapeDtypeStruct((8, width), F32),
        ],
        scratch_shapes=[
            pltpu.VMEM((3, 2, zs, 2, shard, width), BF16),
            pltpu.VMEM((3, zs, 2, 2, shard, width), BF16),
            pltpu.VMEM((3, zs, 2, 2, half, width), BF16),
            pltpu.VMEM((3, zs, 2, half, width), BF16),
            pltpu.VMEM((3, zs - 1, 2, half, width), BF16),
            pltpu.VMEM((HALO, width), BF16),
            pltpu.VMEM((2, 8, width), F32),
            pltpu.VMEM((2, 8, width), F32),
            pltpu.VMEM((8, width), F32),
            pltpu.VMEM((2 * zs - 1, 8, width), F32),
            pltpu.SemaphoreType.DMA((2, 3, zs, 8)),
            pltpu.SemaphoreType.DMA((2, 2 + 2 * zs)),
            pltpu.SemaphoreType.DMA((2,)),
        ],
        compiler_params=pltpu.CompilerParams(
            vmem_limit_bytes=60 * 1024 * 1024, collective_id=1, has_side_effects=True
        ),
        name="reduce",
    )(g_hbm.reshape(3, 2, 2, zs, 2, shard, width), small, passed, resid_grad, own, tokens, gains)


def arrange(q, k, v, o):
    cut = lambda a, h: a[..., h * HD : (h + 1) * HD]
    order = [cut(o, 0), cut(o, 1), cut(o, 2), cut(q, 2), cut(q, 0), cut(q, 1)]
    order += [cut(k, 0), cut(k, 1), cut(v, 0), cut(v, 1), cut(v, 2), cut(k, 2)]
    return jnp.concatenate(order, axis=-1)


def disarrange(a):
    cut = lambda i: a[..., i * HD : (i + 1) * HD]
    join = lambda *ids: jnp.concatenate([cut(i) for i in ids], axis=-1)
    return join(4, 5, 3), join(6, 7, 11), join(8, 9, 10), join(0, 1, 2)


def shards(
    tokens, seg_ids, counts, gain_attn, gain_ffn, w_qkv, dconv_kernel, w_out, w_up, w_down, grad_out
):
    rows, width = tokens.shape
    n_mp = lax.axis_size("mp")
    n_batch = lax.axis_size("batch")
    part = width // n_mp
    shard = w_qkv.shape[0]
    fits = (
        rows % SEQ_MAX == 0 and part == 3 * HD and width == 4 * part and shard % 16 == 0
        and w_up.shape[1] == width and seg_ids.shape[0] == n_mp * rows and shard % 32 == 0 and n_batch % 2 == 0
        and rows + HALO == width
    )
    if not fits:
        return shards_plain(
            tokens, seg_ids, counts, gain_attn, gain_ffn, w_qkv, dconv_kernel, w_out, w_up, w_down, grad_out
        )
    own_start = lax.axis_index("mp") * rows
    piece_a = arrange(w_qkv[:, 0], w_qkv[:, 1], w_qkv[:, 2], w_out.T)
    pieces = jnp.stack([piece_a, w_up, w_down.T])
    taps = lax.all_gather(dconv_kernel, "mp", axis=0, tiled=False)
    zero = jnp.zeros_like(taps[:, 0])
    kernel = arrange(taps[:, 0], taps[:, 1], taps[:, 2], zero)[..., BLK:]
    seg_pad = jnp.concatenate([jnp.full((HALO,), -1, jnp.int32), seg_ids])
    seg = lax.dynamic_slice_in_dim(seg_pad, own_start, HALO + rows, 0).astype(F32)
    slot = own_start - HALO + lax.iota(jnp.int32, HALO + rows)
    cols = jnp.stack(
        [
            (seg == later(seg, 1)).astype(F32).at[0].set(0.0),
            (seg == later(seg, 2)).astype(F32).at[:2].set(0.0),
            seg,
            (slot < counts[0]).astype(F32),
        ],
        axis=1,
    )
    gains = jnp.stack([gain_attn, gain_ffn])
    g, layer_out, resid_grad, own_normed, passed, small = layer_call(
        pieces, tokens, grad_out, cols, seg[None, HALO:], gains, kernel
    )
    own, grad_tokens, small = reduce_call(g, small, passed, resid_grad, own_normed, tokens, gains)
    first, second, third, _ = disarrange(small[:3])
    piece = part // n_batch
    at_piece = lax.axis_index("batch") * piece
    taps_grad = lax.dynamic_slice_in_dim(jnp.stack([first, second, third]), at_piece, piece, 2)
    gain_grads = lax.dynamic_slice_in_dim(small[3:5], lax.axis_index("mp") * part + at_piece, piece, 1)
    q, k, v, o = disarrange(own[0])
    return (
        layer_out,
        grad_tokens,
        gain_grads[0],
        gain_grads[1],
        jnp.stack([q, k, v], axis=1),
        taps_grad,
        o.T,
        own[1],
        own[2].T,
    )


def solution(mesh):
    in_specs = (
        P(("batch", "mp"), None),
        P("batch"),
        P("batch"),
        P(),
        P(),
        P("batch", None, "mp"),
        P(None, None, "mp"),
        P("mp", "batch"),
        P("batch", "mp"),
        P("mp", "batch"),
        P(("batch", "mp"), None),
    )
    out_specs = (
        P(("batch", "mp"), None),
        P(("batch", "mp"), None),
        P(("mp", "batch")),
        P(("mp", "batch")),
        P("batch", None, "mp"),
        P(None, None, ("mp", "batch")),
        P("mp", "batch"),
        P("batch", "mp"),
        P("mp", "batch"),
    )
    return jax.shard_map(shards, mesh=mesh, in_specs=in_specs, out_specs=out_specs, check_vma=False)
```

```python
import jax
import jax.numpy as jnp
from jax import lax
from jax.experimental import pallas as pl
from jax.experimental.pallas import tpu as pltpu
from jax.sharding import PartitionSpec as P

HD = 64
SEQ_MAX = 256
PAD = 16
EPSILON = 1e-06
MASKED = -1e30
F32 = jnp.float32
BF16 = jnp.bfloat16


def nt(left, right):
    return lax.dot_general(left, right, (((1,), (1,)), ((), ())), preferred_element_type=F32)


def nn(left, right):
    return lax.dot_general(left, right, (((1,), (0,)), ((), ())), preferred_element_type=F32)


def tn(left, right):
    return lax.dot_general(left, right, (((0,), (0,)), ((), ())), preferred_element_type=F32)


def head_mask(values, head):
    lane = lax.broadcasted_iota(jnp.int32, values.shape, 1)
    return jnp.where((lane >= head * HD) & (lane < (head + 1) * HD), values, jnp.zeros_like(values))


def attend_kernel(q_ref, k_ref, v_ref, seg_key_ref, seg_query_ref, out_ref, prob_ref, bias_ref):
    tile = SEQ_MAX
    tiles = q_ref.shape[0] // tile

    @pl.when(pl.program_id(0) == 0)
    def _():
        for at in range(tiles):
            key = lax.broadcasted_iota(jnp.int32, (2 * tile, tile), 0)
            query = lax.broadcasted_iota(jnp.int32, (2 * tile, tile), 1) + tile
            same = seg_key_ref[at * tile : (at + 2) * tile, :] == seg_query_ref[:, at * tile : (at + 1) * tile]
            bias_ref[at] = jnp.where(same & (key <= query), 0.0, MASKED).astype(F32)

    for at in range(tiles):
        keys = k_ref[at * tile : (at + 2) * tile, :]
        values = v_ref[at * tile : (at + 2) * tile, :]
        queries = q_ref[at * tile : (at + 1) * tile, :] * jnp.asarray(HD**-0.5, BF16)
        outs = []
        for head in range(2):
            scores = nt(keys, head_mask(queries, head)) + bias_ref[at]
            expo = jnp.exp(scores - jnp.max(scores, axis=0, keepdims=True))
            prob = (expo * (1.0 / jnp.sum(expo, axis=0, keepdims=True))).astype(BF16)
            prob_ref[0, at, head] = prob
            outs.append(tn(head_mask(values, head), prob))
        out_ref[at * tile : (at + 1) * tile, :] = (outs[0] + outs[1]).T.astype(BF16)


def attend_back_kernel(q_ref, k_ref, v_ref, grad_ref, prob_ref, dq_ref, dk_ref, dv_ref):
    tile = SEQ_MAX
    tiles = q_ref.shape[0] // tile
    dk_ref[...] = jnp.zeros_like(dk_ref)
    dv_ref[...] = jnp.zeros_like(dv_ref)
    for at in range(tiles):
        span = slice(at * tile, (at + 2) * tile)
        keys = k_ref[span, :]
        values = v_ref[span, :]
        queries = q_ref[at * tile : (at + 1) * tile, :] * jnp.asarray(HD**-0.5, BF16)
        grads = grad_ref[at * tile : (at + 1) * tile, :]
        dq = 0.0
        for head in range(2):
            prob = prob_ref[0, at, head]
            grad_head = head_mask(grads, head)
            grad_prob = nt(values, grad_head)
            wide = prob.astype(F32)
            inner = wide * grad_prob
            grad_scores = (inner - wide * jnp.sum(inner, axis=0, keepdims=True)).astype(BF16)
            dv_ref[span, :] += nn(prob, grad_head)
            dk_ref[span, :] += nn(grad_scores, head_mask(queries, head))
            dq = dq + tn(head_mask(keys, head), grad_scores)
        dq_ref[at * tile : (at + 1) * tile, :] = (dq * HD**-0.5).T


def attend(queries, keys, values, seg_key, seg_query):
    rows, width = queries.shape
    span = keys.shape[0]
    tiles = rows // SEQ_MAX
    wide = 2 * HD
    return pl.pallas_call(
        attend_kernel,
        grid=(width // wide,),
        in_specs=[
            pl.BlockSpec((rows, wide), lambda i: (0, i)),
            pl.BlockSpec((span, wide), lambda i: (0, i)),
            pl.BlockSpec((span, wide), lambda i: (0, i)),
            pl.BlockSpec((span, 1), lambda i: (0, 0)),
            pl.BlockSpec((1, rows), lambda i: (0, 0)),
        ],
        out_specs=[
            pl.BlockSpec((rows, wide), lambda i: (0, i)),
            pl.BlockSpec((1, tiles, 2, 2 * SEQ_MAX, SEQ_MAX), lambda i: (i, 0, 0, 0, 0)),
        ],
        out_shape=[
            jax.ShapeDtypeStruct((rows, width), BF16),
            jax.ShapeDtypeStruct((width // wide, tiles, 2, 2 * SEQ_MAX, SEQ_MAX), BF16),
        ],
        scratch_shapes=[pltpu.VMEM((tiles, 2 * SEQ_MAX, SEQ_MAX), F32)],
        name="attend",
    )(queries, keys, values, seg_key[:, None], seg_query[None, :])


def attend_back(queries, keys, values, grads, prob):
    rows, width = queries.shape
    span = keys.shape[0]
    tiles = rows // SEQ_MAX
    wide = 2 * HD
    return pl.pallas_call(
        attend_back_kernel,
        grid=(width // wide,),
        in_specs=[
            pl.BlockSpec((rows, wide), lambda i: (0, i)),
            pl.BlockSpec((span, wide), lambda i: (0, i)),
            pl.BlockSpec((span, wide), lambda i: (0, i)),
            pl.BlockSpec((rows, wide), lambda i: (0, i)),
            pl.BlockSpec((1, tiles, 2, 2 * SEQ_MAX, SEQ_MAX), lambda i: (i, 0, 0, 0, 0)),
        ],
        out_specs=[
            pl.BlockSpec((rows, wide), lambda i: (0, i)),
            pl.BlockSpec((span, wide), lambda i: (0, i)),
            pl.BlockSpec((span, wide), lambda i: (0, i)),
        ],
        out_shape=[
            jax.ShapeDtypeStruct((rows, width), F32),
            jax.ShapeDtypeStruct((span, width), F32),
            jax.ShapeDtypeStruct((span, width), F32),
        ],
        name="attend_back",
    )(queries, keys, values, grads, prob)


def rms(values):
    return lax.rsqrt(jnp.mean(values * values, axis=-1, keepdims=True) + EPSILON)


def rms_back(grad, gain, hat, scale):
    scaled = grad * gain
    return scale * (scaled - hat * jnp.mean(scaled * hat, axis=-1, keepdims=True))


def later(values, by):
    return jnp.concatenate([jnp.zeros((by,) + values.shape[1:], values.dtype), values[:-by]], axis=0)


def sooner(values, by):
    return jnp.concatenate([values[by:], jnp.zeros((by,) + values.shape[1:], values.dtype)], axis=0)


def shards_plain(
    tokens, seg_ids, counts, gain_attn, gain_ffn, w_qkv, dconv_kernel, w_out, w_up, w_down, grad_out
):
    rows, width = tokens.shape
    halo = SEQ_MAX + PAD
    n_mp = lax.axis_size("mp")
    n_batch = lax.axis_size("batch")
    part = width // n_mp
    ff = w_up.shape[1] * n_mp
    own_start = lax.axis_index("mp") * rows

    packed = jnp.concatenate(
        [w_qkv.reshape(w_qkv.shape[0], -1), w_out.T, w_up, w_down.T], axis=1
    )
    full = lax.all_gather(packed, ("batch", "mp"), axis=0, tiled=False)
    full = full.reshape((n_batch, n_mp) + packed.shape).transpose(0, 2, 1, 3).reshape(width, n_mp, -1)
    cuts = (3 * part, 4 * part, 4 * part + w_up.shape[1])
    full_qkv = full[:, :, : cuts[0]].reshape(width, n_mp, 3, part).transpose(0, 2, 1, 3).reshape(width, 3 * width)
    full_out = full[:, :, cuts[0] : cuts[1]].reshape(width, width)
    full_up = full[:, :, cuts[1] : cuts[2]].reshape(width, ff)
    full_down = full[:, :, cuts[2] :].reshape(width, ff)
    kernel = lax.all_gather(dconv_kernel, "mp", axis=2, tiled=True).transpose(1, 0, 2).reshape(3, 3 * width)

    back = [(i, i + 1) for i in range(n_mp - 1)]
    tok_halo = lax.ppermute(tokens[rows - halo :], "mp", back)
    ext = jnp.concatenate([tok_halo, tokens], axis=0).astype(F32)
    seg_pad = jnp.concatenate([jnp.full((halo,), -1, jnp.int32), seg_ids])
    seg = lax.dynamic_slice_in_dim(seg_pad, own_start, halo + rows, 0)
    same_one = (seg == later(seg, 1)).astype(F32)[:, None]
    same_two = (seg == later(seg, 2)).astype(F32)[:, None]
    slot = own_start + lax.iota(jnp.int32, rows)
    filled = (slot < counts[0]).astype(F32)[:, None]

    scale_one = rms(ext)
    hat_one = ext * scale_one
    normed = (hat_one * gain_attn).astype(BF16)
    projected = nn(normed, full_qkv)
    mixed = (
        kernel[0] * projected
        + kernel[1] * same_one * later(projected, 1)
        + kernel[2] * same_two * later(projected, 2)
    ).astype(BF16)
    queries = mixed[halo:, :width]
    keys = mixed[PAD:, width : 2 * width]
    values = mixed[PAD:, 2 * width :]
    heads, prob = attend(queries, keys, values, seg[PAD:], seg[halo:])
    residual = ext[halo:] + filled * nn(heads, full_out.T if False else full_out.T)
    scale_two = rms(residual)
    hat_two = residual * scale_two
    normed_two = (hat_two * gain_ffn).astype(BF16)
    up = jax.nn.relu(nn(normed_two, full_up))
    hidden = (up * up).astype(BF16)
    layer_out = (residual + filled * nt(hidden, full_down)).astype(BF16)

    grad = grad_out.astype(F32)
    grad_ffn = (filled * grad).astype(BF16)
    grad_up = (nn(grad_ffn, full_down) * 2.0 * up).astype(BF16)
    grad_w_down = tn(grad_ffn, hidden)
    grad_w_up = tn(normed_two, grad_up)
    grad_normed_two = nt(grad_up, full_up)
    grad_resid = grad + rms_back(grad_normed_two, gain_ffn, hat_two, scale_two)
    grad_gain_ffn = jnp.sum(grad_normed_two * hat_two, axis=0)
    grad_attn = (filled * grad_resid).astype(BF16)
    grad_w_out = tn(grad_attn, heads)
    grad_heads = nn(grad_attn, full_out).astype(BF16)
    dq, dk, dv = attend_back(queries, keys, values, grad_heads, prob)
    grad_mixed = jnp.concatenate(
        [
            jnp.pad(dq, ((halo, 0), (0, 0))),
            jnp.pad(dk, ((PAD, 0), (0, 0))),
            jnp.pad(dv, ((PAD, 0), (0, 0))),
        ],
        axis=1,
    )
    one = grad_mixed * same_one
    two = grad_mixed * same_two
    grad_kernel = jnp.stack(
        [
            jnp.sum(grad_mixed * projected, axis=0),
            jnp.sum(one * later(projected, 1), axis=0),
            jnp.sum(two * later(projected, 2), axis=0),
        ]
    )
    grad_proj = (
        kernel[0] * grad_mixed + kernel[1] * sooner(one, 1) + kernel[2] * sooner(two, 2)
    ).astype(BF16)
    grad_w_qkv = tn(normed, grad_proj)
    grad_normed = nt(grad_proj, full_qkv)
    ahead = [(i + 1, i) for i in range(n_mp - 1)]
    passed = lax.ppermute(grad_normed[:halo].astype(BF16), "mp", ahead).astype(F32)
    own_normed = grad_normed[halo:] + jnp.pad(passed, ((rows - halo, 0), (0, 0)))
    grad_tokens = grad_resid + rms_back(own_normed, gain_attn, hat_one[halo:], scale_one[halo:])
    grad_gain_attn = jnp.sum(own_normed * hat_one[halo:], axis=0)

    shard = packed.shape[0]
    grads = jnp.concatenate(
        [
            grad_w_qkv.astype(BF16).reshape(width, 3, n_mp, part).transpose(0, 2, 1, 3).reshape(width, n_mp, -1),
            grad_w_out.astype(BF16).reshape(width, n_mp, -1),
            grad_w_up.astype(BF16).reshape(width, n_mp, -1),
            grad_w_down.astype(BF16).reshape(width, n_mp, -1),
        ],
        axis=2,
    )
    grads = grads.reshape(n_batch, shard, n_mp, -1).transpose(0, 2, 1, 3).reshape(n_batch * n_mp, shard, -1)
    own = lax.psum_scatter(grads, ("batch", "mp"), scatter_dimension=0, tiled=False).astype(F32)
    small = jnp.concatenate(
        [grad_kernel.reshape(3, 3, width).transpose(1, 0, 2).reshape(9, width), grad_gain_attn[None], grad_gain_ffn[None]]
    )
    piece = width // (n_mp * n_batch)
    small = small.reshape(11, n_mp * n_batch, piece).transpose(1, 0, 2)
    small = lax.psum_scatter(small, ("mp", "batch"), scatter_dimension=0, tiled=False)
    return (
        layer_out,
        grad_tokens,
        small[9],
        small[10],
        own[:, : cuts[0]].reshape(shard, 3, part),
        small[:9].reshape(3, 3, piece),
        own[:, cuts[0] : cuts[1]].T,
        own[:, cuts[1] : cuts[2]],
        own[:, cuts[2] :].T,
    )


HALO = SEQ_MAX
BLK = 128
HEADS = ((1, 2, 3, False, False, 0), (1, 2, 3, True, True, 0), (0, 4, 4, True, False, 1))
COLUMNS = 5 * BLK


def blk(index):
    return slice(index * BLK, (index + 1) * BLK)


def half_of(values, upper):
    lane = lax.broadcasted_iota(jnp.int32, values.shape, 1)
    keep = (lane >= HD) if upper else (lane < HD)
    return jnp.where(keep, values, jnp.zeros_like(values))


def rows_loop(total, size, body):
    def one(i, carry):
        body(pl.ds(pl.multiple_of(i * size, size), size))
        return carry

    lax.fori_loop(0, total // size, one, 0)


def parts_loop(count, body):
    def one(i, carry):
        body(i)
        return carry

    lax.fori_loop(0, count, one, 0)


MESH = pl.DeviceIdType.MESH


def meet_all():
    barrier = pltpu.get_barrier_semaphore()
    others = 0
    for axis in ("batch", "mp"):
        size = lax.axis_size(axis)
        for by in range(1, size):
            other = lax.rem(lax.axis_index(axis) + by, size)
            pl.semaphore_signal(barrier, inc=1, device_id={axis: other}, device_id_type=MESH)
        others += size - 1
    pl.semaphore_wait(barrier, others)


class Place:
    def __init__(self):
        self.b = lax.axis_index("batch")
        self.m = lax.axis_index("mp")
        self.zs = lax.axis_size("batch") // 2
        self.z = self.b // 2
        self.y = lax.rem(self.b, 2)

    def behind(self, k):
        return lax.rem(self.z + self.zs - k, self.zs) * 2

    def ahead(self, k):
        return lax.rem(self.z + k, self.zs) * 2

    def flip_x(self):
        return lax.rem(self.m + 2, 4)

    def flip_core(self, m):
        return m + 1 - 2 * lax.rem(m, 2)


class Gather:
    def __init__(self, pieces, w, send_sems, recv_sems, own_sems):
        self.pieces, self.w, self.send, self.recv, self.own = pieces, w, send_sems, recv_sems, own_sems
        self.at = Place()
        self.shard = pieces.shape[1]
        self.half = self.shard // 2

    def spot(self, p, c, k, j, core=False):
        at = self.at
        cross_y = j in ((1, 3) if c == 0 else (2, 3))
        cross_x = j in ((2, 3) if c == 0 else (1, 3))
        b = at.behind(k) + (1 - at.y if cross_y else at.y)
        m = at.flip_x() if cross_x else at.m
        m = at.flip_core(m) if core else m
        half = slice(c * self.half, (c + 1) * self.half)
        return self.w.at[p, m // 2, lax.rem(m, 2), b // 2, lax.rem(b, 2), half, :]

    def copy(self, p, c, k, j, number, target, core=False):
        own = self.pieces.at[p, c * self.half : (c + 1) * self.half, :]
        return pltpu.make_async_remote_copy(
            own if (k, j) == (0, 0) else self.spot(p, c, k, j),
            self.spot(p, c, k, j),
            self.send.at[p, c, number],
            self.recv.at[p, c, number],
            device_id=target,
            device_id_type=MESH,
        )

    def to(self, axis):
        at = self.at
        return {"batch": at.z * 2 + 1 - at.y} if axis == "y" else {"mp": at.flip_x()}

    def along_z(self, p, c):
        return [
            self.copy(p, c, 0, 0, by - 1, {"batch": self.at.ahead(by) + self.at.y}) for by in range(1, self.at.zs)
        ]

    def hops(self, p, c, k, j):
        zs = self.at.zs
        axes = ("y", "x") if c == 0 else ("x", "y")
        out = []
        if j == 0:
            out.append(self.copy(p, c, k, j, zs - 1 + k, self.to(axes[0])))
        if j in (0, 1):
            out.append(self.copy(p, c, k, j, 2 * zs - 1 + 2 * k + j, self.to(axes[1])))
        out.append(self.copy(p, c, k, j, 4 * zs - 1 + 4 * k + j, {"mp": self.at.flip_core(self.at.m)}))
        return out

    def arrived(self, p, c, k, j):
        zs = self.at.zs
        number = (k - 1, zs - 1 + k, 2 * zs - 1 + 2 * k, 2 * zs + 2 * k)[j]
        self.wait(p, c, number, self.spot(p, c, k, j))

    def wait(self, p, c, number, ref):
        pltpu.make_async_copy(ref, ref, self.recv.at[p, c, number]).wait()

    def keep(self, p):
        at = self.at
        own = self.w.at[p, at.m // 2, lax.rem(at.m, 2), at.z, at.y]
        return pltpu.make_async_copy(self.pieces.at[p], own, self.own.at[p])

    def begin_z(self, p):
        self.keep(p).start()
        copies = [self.along_z(p, c) for c in range(2)]
        for by in range(self.at.zs - 1):
            for c in range(2):
                copies[c][by].start()

    def begin(self, p):
        for c in range(2):
            for hop in self.hops(p, c, 0, 0):
                hop.start()

    def relay(self, p, j):
        for k in range(self.at.zs):
            for c in range(2):
                if (k, j) != (0, 0):
                    self.arrived(p, c, k, j)
                    for hop in self.hops(p, c, k, j):
                        hop.start()

    def finish(self, p):
        self.keep(p).wait()
        for k in range(self.at.zs):
            for j in range(4):
                for c in range(2):
                    self.wait(p, c, 4 * self.at.zs - 1 + 4 * k + j, self.spot(p, c, k, j, core=True))

    def drain(self, p):
        for c in range(2):
            for copy in self.along_z(p, c):
                copy.wait_send()
            for k in range(self.at.zs):
                for j in range(4):
                    for hop in self.hops(p, c, k, j):
                        hop.wait_send()


class Reduce:
    def __init__(self, w, one, two, three, four, one_sems, sems):
        self.w, self.one, self.two, self.three, self.four, self.one_sems, self.sems = (
            w, one, two, three, four, one_sems, sems
        )
        self.at = Place()
        self.x = self.at.m // 2
        self.core = lax.rem(self.at.m, 2)
        self.half = w.shape[5] // 2

    def z(self, k):
        return self.at.ahead(k) // 2

    def lanes(self, c):
        return slice(c * self.half, (c + 1) * self.half)

    def remote(self, source, target, sems, number, device):
        return pltpu.make_async_remote_copy(
            source, target, sems.at[(0,) + number], sems.at[(1,) + number], device_id=device, device_id_type=MESH
        )

    def first(self, p, x):
        other = {"mp": self.at.flip_core(self.at.m)}
        return self.remote(self.w.at[p, x, 1 - self.core], self.one.at[p, x], self.one_sems, (p, x), other)

    def second(self, p, k, c):
        z, at = self.z(k), self.at
        if c == 0:
            source, device = self.w.at[p, 1 - self.x, self.core, z, :, self.lanes(0), :], {"mp": at.flip_x()}
        else:
            source = self.w.at[p, :, self.core, z, 1 - at.y, self.lanes(1), :]
            device = {"batch": at.z * 2 + 1 - at.y}
        return self.remote(source, self.two.at[p, k, c], self.sems, (p, k, c), device)

    def third(self, p, k, c):
        z, at = self.z(k), self.at
        if c == 0:
            source = self.w.at[p, self.x, self.core, z, 1 - at.y, self.lanes(0), :]
            device = {"batch": at.z * 2 + 1 - at.y}
        else:
            source, device = self.w.at[p, 1 - self.x, self.core, z, at.y, self.lanes(1), :], {"mp": at.flip_x()}
        return self.remote(source, self.three.at[p, k, c], self.sems, (p, k, 2 + c), device)

    def fourth(self, p, k, c):
        at = self.at
        source = self.w.at[p, self.x, self.core, self.z(k), at.y, self.lanes(c), :]
        return self.remote(source, self.four.at[p, k - 1, c], self.sems, (p, k, 4 + c), {"batch": at.ahead(k) + at.y})

    def start(self, p):
        for x in range(2):
            self.first(p, x).start()

    def met(self, p):
        for x in range(2):
            self.first(p, x).wait_recv()

    def step_one(self, p, k):
        z = self.z(k)
        for x in range(2):
            self.w[p, x, self.core, z] += self.one[p, x, z]
        for c in range(2):
            self.second(p, k, c).start()

    def step_two(self, p, k):
        z, at = self.z(k), self.at
        self.second(p, k, 0).wait_recv()
        for y in range(2):
            self.w[p, self.x, self.core, z, y, self.lanes(0), :] += self.two[p, k, 0, y]
        self.third(p, k, 0).start()
        self.second(p, k, 1).wait_recv()
        for x in range(2):
            self.w[p, x, self.core, z, at.y, self.lanes(1), :] += self.two[p, k, 1, x]
        self.third(p, k, 1).start()

    def step_three(self, p, k):
        z, at = self.z(k), self.at
        for c in range(2):
            self.third(p, k, c).wait_recv()
            self.w[p, self.x, self.core, z, at.y, self.lanes(c), :] += self.three[p, k, c]
            if k:
                self.fourth(p, k, c).start()

    def step_four(self, p, out):
        for c in range(2):
            total = self.w[p, self.x, self.core, self.at.z, self.at.y, self.lanes(c), :].astype(F32)
            for k in range(1, self.at.zs):
                self.fourth(p, k, c).wait_recv()
                total = total + self.four[p, k - 1, c].astype(F32)
            out[p, self.lanes(c), :] = total

    def drain(self, p):
        for x in range(2):
            self.first(p, x).wait_send()
        for k in range(self.at.zs):
            for c in range(2):
                self.second(p, k, c).wait_send()
                self.third(p, k, c).wait_send()
                if k:
                    self.fourth(p, k, c).wait_send()


class Small:
    def __init__(self, source, one, two, three, sums, sems):
        self.source, self.one, self.two, self.three, self.sums, self.sems = source, one, two, three, sums, sems
        self.at = Place()
        self.x = self.at.m // 2
        self.core = lax.rem(self.at.m, 2)
        self.count = lax.axis_size("batch")

    def remote(self, source, target, number, device):
        return pltpu.make_async_remote_copy(
            source, target, self.sems.at[0, number], self.sems.at[1, number], device_id=device, device_id_type=MESH
        )

    def core_copy(self, x):
        device = {"mp": self.at.flip_core(self.at.m)}
        return self.remote(self.source.at[x * 2 + 1 - self.core], self.one.at[x], x, device)

    def x_copy(self):
        return self.remote(self.sums.at[1 - self.x], self.two, 2, {"mp": self.at.flip_x()})

    def far_copy(self, by):
        other = lax.rem(self.at.b + by, self.count)
        return self.remote(self.sums.at[self.x], self.three.at[by - 1], 2 + by, {"batch": other})

    def begin(self):
        for x in range(2):
            self.core_copy(x).start()

    def middle(self):
        for x in range(2):
            self.core_copy(x).wait_recv()
            self.sums[x] = self.source[x * 2 + self.core] + self.one[x]
        self.x_copy().start()

    def later(self):
        self.x_copy().wait_recv()
        self.sums[self.x] += self.two[...]
        for by in range(1, self.count):
            self.far_copy(by).start()

    def finish(self, out):
        total = self.sums[self.x]
        for by in range(1, self.count):
            self.far_copy(by).wait_recv()
            total = total + self.three[by - 1]
        out[...] = total
        for x in range(2):
            self.core_copy(x).wait_send()
        self.x_copy().wait_send()
        for by in range(1, self.count):
            self.far_copy(by).wait_send()


def layer_kernel(
    pieces_ref, tok_ref, grad_ref, cols_ref, seg_row_ref, gains_ref, kernel_ref,
    out_ref, tokens_out, own_out, small_out,
    w, ext_ref, normed, proj, mixed, prob, heads, bias, wide, acc, own_ref, normed_two,
    gffn_t, two_t, hidden, upper, one, two, three, four, sent, passed,
    small_ref, s_sums, s_one, s_two, s_three,
    send_sems, recv_sems, own_sems, halo_sems, one_sems, sems, small_sems,
):
    parts = w.shape[1] * w.shape[2]
    rows, width = tokens_out.shape
    span = HALO + rows
    tiles = rows // SEQ_MAX
    tile = SEQ_MAX
    resid = tokens_out
    me = lax.axis_index("mp")
    pull = Gather(pieces_ref, w, send_sems, recv_sems, own_sems)
    push = Reduce(w, one, two, three, four, one_sems, sems)
    small = Small(small_ref, s_one, s_two, s_three, s_sums, small_sems)
    zs = push.at.zs
    ks = [*range(1, zs), 0]

    def weight(piece, m):
        return w[piece, m // 2, lax.rem(m, 2)].reshape(width, width)

    def store(piece, m, lanes, value):
        w[piece, m // 2, lax.rem(m, 2), :, :, :, lanes] = value.reshape(zs, 2, width // (2 * zs), value.shape[1])

    def lanes_of(piece, m, lanes):
        value = w[piece, m // 2, lax.rem(m, 2), :, :, :, lanes]
        return value.reshape(width, value.shape[3])

    def neighbour(source, target, first, by):
        return pltpu.make_async_remote_copy(
            source, target, halo_sems.at[first], halo_sems.at[first + 1],
            device_id={"mp": lax.rem(me + by, parts)}, device_id_type=MESH,
        )

    meet_all()
    pull.begin_z(0)
    pull.begin(0)
    pass_on = neighbour(tok_ref.at[rows - HALO :], ext_ref.at[:HALO], 0, 1)
    pass_on.start()
    pull.begin_z(1)
    pull.begin_z(2)
    ext_ref[HALO:, :] = tok_ref[...]

    gain_one = gains_ref[0:1, :]
    gain_two = gains_ref[1:2, :]

    def norm_one(at):
        values = ext_ref[at, :].astype(F32)
        normed[at, :] = (values * rms(values) * gain_one).astype(BF16)

    pass_on.wait()
    rows_loop(span, 128, norm_one)
    for at in range(tiles):
        key = lax.broadcasted_iota(jnp.int32, (2 * tile, tile), 0)
        query = lax.broadcasted_iota(jnp.int32, (2 * tile, tile), 1) + tile
        seg_key = cols_ref[at * tile : (at + 2) * tile, 2:3]
        same = seg_key == seg_row_ref[0:1, at * tile : (at + 1) * tile]
        bias[at] = jnp.where(same & (key <= query), 0.0, MASKED).astype(BF16)
    acc[...] = jnp.zeros_like(acc)

    def forward(m):
        wide[...] = nn(normed[...], lanes_of(0, m, slice(BLK, width)))
        for c in range(5):
            source = wide[:, blk(c)]
            proj[m, :, blk(c)] = source.astype(BF16)
            mixed[m, :, blk(c)] = (
                kernel_ref[m, 0:1, blk(c)] * source
                + kernel_ref[m, 1:2, blk(c)] * (cols_ref[:, 0:1] * pltpu.roll(source, 1, 0))
                + kernel_ref[m, 2:3, blk(c)] * (cols_ref[:, 1:2] * pltpu.roll(source, 2, 0))
            ).astype(BF16)
        for at in range(tiles):
            keys_at = slice(at * tile, (at + 2) * tile)
            query_at = slice(HALO + at * tile, HALO + (at + 1) * tile)
            outs = []
            for h, (qb, kb, vb, qk_upper, v_upper, _) in enumerate(HEADS):
                queries = half_of(mixed[m, query_at, blk(qb)], qk_upper) * jnp.asarray(HD**-0.5, BF16)
                scores = nt(mixed[m, keys_at, blk(kb)], queries) + bias[at].astype(F32)
                expo = jnp.exp(scores - jnp.max(scores, axis=0, keepdims=True))
                share = (expo * (1.0 / jnp.sum(expo, axis=0, keepdims=True))).astype(BF16)
                prob[m, at, h] = share
                outs.append(tn(half_of(mixed[m, keys_at, blk(vb)], v_upper), share))
            own_at = slice(at * tile, (at + 1) * tile)
            heads[m, own_at, blk(0)] = (outs[0] + outs[1]).T.astype(BF16)
            heads[m, own_at, blk(1)] = outs[2].T.astype(BF16)
        acc[...] += nt(heads[m], lanes_of(0, m, slice(0, 2 * BLK)))

        @pl.when(m == 1)
        def _():
            pull.relay(1, 1)
            pull.begin(2)
            pull.relay(2, 0)

        @pl.when(m == 2)
        def _():
            pull.relay(1, 2)
            pull.relay(1, 3)

    pull.relay(0, 0)
    pull.begin(1)
    for j in range(1, 4):
        pull.relay(0, j)
    pull.finish(0)
    pull.relay(1, 0)
    parts_loop(parts, forward)
    pull.relay(2, 1)

    def middle(at):
        values = ext_ref[pl.ds(at.start + HALO, at.size), :].astype(F32)
        filled = cols_ref[pl.ds(at.start + HALO, at.size), 3:4]
        value = values + filled * acc[at, :]
        resid[at, :] = value
        normed_two[at, :] = (value * rms(value) * gain_two).astype(BF16)
        out_ref[at, :] = (filled * grad_ref[at, :].astype(F32)).astype(BF16)

    rows_loop(rows, 128, middle)
    gffn = out_ref
    gffn_t[...] = gffn[...].T
    two_t[...] = normed_two[...].T
    normed[...] = normed[...].T
    normed_t = normed
    acc[...] = jnp.zeros_like(acc)
    own_ref[...] = jnp.zeros_like(own_ref)
    pull.relay(2, 2)
    pull.relay(2, 3)
    for p in (1, 2):
        pull.finish(p)
    for p in range(3):
        pull.drain(p)

    def feed(m):
        up = jnp.maximum(nn(normed_two[...], weight(1, m)), 0.0)
        upper[...] = (2.0 * up).astype(BF16)
        hidden[...] = (up * up).astype(BF16)
        acc[...] += nt(hidden[...], weight(2, m))
        upper[...] = (nn(gffn[...], weight(2, m)) * upper[...].astype(F32)).astype(BF16)
        store(2, m, slice(0, width), nn(gffn_t[...], hidden[...]).astype(BF16))
        own_ref[...] += nt(upper[...], weight(1, m))
        store(1, m, slice(0, width), nn(two_t[...], upper[...]).astype(BF16))

    parts_loop(parts, feed)
    push.start(2)
    push.start(1)

    small_ref[...] = jnp.zeros_like(small_ref)

    def turn(at):
        value = resid[at, :]
        filled = cols_ref[pl.ds(at.start + HALO, at.size), 3:4]
        scale = rms(value)
        hat = value * scale
        grad = own_ref[at, :]
        small_ref[0, 4:5, :] += jnp.sum(grad * hat, axis=0, keepdims=True)
        total = grad_ref[at, :].astype(F32) + rms_back(grad, gain_two, hat, scale)
        tokens_out[at, :] = total
        out_ref[at, :] = (value + filled * acc[at, :]).astype(BF16)
        normed_two[at, :] = (filled * total).astype(BF16)

    rows_loop(rows, 128, turn)
    gattn = normed_two
    two_t[...] = gattn[...].T
    own_ref[...] = jnp.zeros_like(own_ref)
    acc[...] = jnp.zeros_like(acc)

    def backward(m):
        @pl.when(m == 0)
        def _():
            push.met(2)
            for k in ks:
                push.step_one(2, k)

        @pl.when(m == 1)
        def _():
            push.met(1)
            for k in ks:
                push.step_one(1, k)

        @pl.when(m == 3)
        def _():
            for k in ks:
                push.step_two(2, k)

        grads = nn(gattn[...], lanes_of(0, m, slice(0, 2 * BLK))).astype(BF16)
        hidden[:, : 2 * BLK] = grads
        wide[...] = jnp.zeros_like(wide)
        for at in range(tiles):
            keys_at = slice(at * tile, (at + 2) * tile)
            query_at = slice(HALO + at * tile, HALO + (at + 1) * tile)
            own_at = slice(at * tile, (at + 1) * tile)
            for h, (qb, kb, vb, qk_upper, v_upper, ob) in enumerate(HEADS):
                share = prob[m, at, h]
                grad_head = half_of(hidden[own_at, blk(ob)], v_upper)
                queries = half_of(mixed[m, query_at, blk(qb)], qk_upper) * jnp.asarray(HD**-0.5, BF16)
                grad_prob = nt(mixed[m, keys_at, blk(vb)], grad_head)
                broad = share.astype(F32)
                inner = broad * grad_prob
                grad_scores = (inner - broad * jnp.sum(inner, axis=0, keepdims=True)).astype(BF16)
                wide[keys_at, blk(vb)] += nn(share, grad_head)
                wide[keys_at, blk(kb)] += nn(grad_scores, queries)
                keys = half_of(mixed[m, keys_at, blk(kb)], qk_upper)
                wide[query_at, blk(qb)] += (tn(keys, grad_scores) * HD**-0.5).T
        for c in range(5):
            grad = wide[:, blk(c)]
            one = grad * cols_ref[:, 0:1]
            two = grad * cols_ref[:, 1:2]
            source = proj[m, :, blk(c)].astype(F32)
            small_ref[m, 0:1, blk(c + 1)] = jnp.sum(grad * source, axis=0, keepdims=True)
            small_ref[m, 1:2, blk(c + 1)] = jnp.sum(one * pltpu.roll(source, 1, 0), axis=0, keepdims=True)
            small_ref[m, 2:3, blk(c + 1)] = jnp.sum(two * pltpu.roll(source, 2, 0), axis=0, keepdims=True)
            mixed[m, :, blk(c)] = (
                kernel_ref[m, 0:1, blk(c)] * grad
                + kernel_ref[m, 1:2, blk(c)] * pltpu.roll(one, span - 1, 0)
                + kernel_ref[m, 2:3, blk(c)] * pltpu.roll(two, span - 2, 0)
            ).astype(BF16)
        own_ref[...] += nt(mixed[m, HALO:, :], lanes_of(0, m, slice(BLK, width)))
        acc[:HALO, :] += nt(mixed[m, :HALO, :], lanes_of(0, m, slice(BLK, width)))
        part = nn(two_t[...], heads[m])
        wide[...] = nn(normed_t[...], mixed[m])
        store(0, m, blk(0), part[:, blk(0)].astype(BF16))
        store(0, m, blk(1), (half_of(part[:, blk(1)], False) + half_of(wide[:, blk(0)], True)).astype(BF16))
        store(0, m, slice(2 * BLK, width), wide[:, BLK:].astype(BF16))

    parts_loop(parts, backward)
    push.start(0)
    sent[...] = acc[:HALO, :].astype(BF16)

    def gain_rows(at, grad):
        values = ext_ref[at, :].astype(F32)
        small_ref[0, 3:4, :] += jnp.sum(grad * (values * rms(values)), axis=0, keepdims=True)

    rows_loop(HALO, 128, lambda at: gain_rows(at, acc[at, :]))
    rows_loop(rows, 128, lambda at: gain_rows(pl.ds(at.start + HALO, at.size), own_ref[at, :]))
    for m in range(1, parts):
        small_ref[m, 3:5, :] = small_ref[0, 3:5, :]
    back_on = neighbour(sent, passed, 2, parts - 1)
    back_on.start()
    small.begin()
    push.met(0)
    for k in ks:
        push.step_one(0, k)
        push.step_two(1, k)
    small.middle()

    def last(at, extra):
        values = tok_ref[at, :].astype(F32)
        scale = rms(values)
        tokens_out[at, :] += rms_back(own_ref[at, :] + extra, gain_one, values * scale, scale)

    def end_rows(at):
        keep = jnp.where(me < parts - 1, 1.0, 0.0)
        last(pl.ds(at.start + rows - HALO, at.size), passed[at, :].astype(F32) * keep)

    rows_loop(rows - HALO, 128, lambda at: last(at, 0.0))
    small.later()
    for k in ks:
        push.step_three(2, k)
        push.step_two(0, k)
        push.step_three(1, k)
    back_on.wait()
    rows_loop(HALO, 128, end_rows)
    push.step_four(2, own_out)
    for k in ks:
        push.step_three(0, k)
    push.step_four(1, own_out)
    small.finish(small_out)
    push.step_four(0, own_out)
    for p in range(3):
        push.drain(p)


def layer_call(pieces, tokens, grad_out, cols, seg_row, gains, kernel):
    parts = lax.axis_size("mp")
    rows, width = grad_out.shape
    span = rows + HALO
    tiles = rows // SEQ_MAX
    zs = lax.axis_size("batch") // 2
    copies = 8 * zs - 1
    shard = width // (2 * zs)
    half = shard // 2
    vmem = pl.BlockSpec(memory_space=pltpu.VMEM)
    return pl.pallas_call(
        layer_kernel,
        in_specs=[vmem] * 7,
        out_specs=[vmem] * 4,
        out_shape=[
            jax.ShapeDtypeStruct((rows, width), BF16),
            jax.ShapeDtypeStruct((rows, width), F32),
            jax.ShapeDtypeStruct((3, shard, width), F32),
            jax.ShapeDtypeStruct((8, width), F32),
        ],
        scratch_shapes=[
            pltpu.VMEM((3, 2, 2, zs, 2, shard, width), BF16),
            pltpu.VMEM((span, width), BF16),
            pltpu.VMEM((span, width), BF16),
            pltpu.VMEM((parts, span, COLUMNS), BF16),
            pltpu.VMEM((parts, span, COLUMNS), BF16),
            pltpu.VMEM((parts, tiles, 3, 2 * SEQ_MAX, SEQ_MAX), BF16),
            pltpu.VMEM((parts, rows, 2 * BLK), BF16),
            pltpu.VMEM((tiles, 2 * SEQ_MAX, SEQ_MAX), BF16),
            pltpu.VMEM((span, COLUMNS), F32),
            pltpu.VMEM((rows, width), F32),
            pltpu.VMEM((rows, width), F32),
            pltpu.VMEM((rows, width), BF16),
            pltpu.VMEM((width, rows), BF16),
            pltpu.VMEM((width, rows), BF16),
            pltpu.VMEM((rows, width), BF16),
            pltpu.VMEM((rows, width), BF16),
            pltpu.VMEM((3, 2, zs, 2, shard, width), BF16),
            pltpu.VMEM((3, zs, 2, 2, half, width), BF16),
            pltpu.VMEM((3, zs, 2, half, width), BF16),
            pltpu.VMEM((3, zs - 1, 2, half, width), BF16),
            pltpu.VMEM((HALO, width), BF16),
            pltpu.VMEM((HALO, width), BF16),
            pltpu.VMEM((parts, 8, width), F32),
            pltpu.VMEM((2, 8, width), F32),
            pltpu.VMEM((2, 8, width), F32),
            pltpu.VMEM((8, width), F32),
            pltpu.VMEM((2 * zs - 1, 8, width), F32),
            pltpu.SemaphoreType.DMA((3, 2, copies)),
            pltpu.SemaphoreType.DMA((3, 2, copies)),
            pltpu.SemaphoreType.DMA((3,)),
            pltpu.SemaphoreType.DMA((4,)),
            pltpu.SemaphoreType.DMA((2, 3, 2)),
            pltpu.SemaphoreType.DMA((2, 3, zs, 6)),
            pltpu.SemaphoreType.DMA((2, 2 + 2 * zs)),
        ],
        compiler_params=pltpu.CompilerParams(
            vmem_limit_bytes=67043328, collective_id=0, has_side_effects=True
        ),
        name="layer",
    )(pieces, tokens, grad_out, cols, seg_row, gains, kernel)


def arrange(q, k, v, o):
    cut = lambda a, h: a[..., h * HD : (h + 1) * HD]
    order = [cut(o, 0), cut(o, 1), cut(o, 2), cut(q, 2), cut(q, 0), cut(q, 1)]
    order += [cut(k, 0), cut(k, 1), cut(v, 0), cut(v, 1), cut(v, 2), cut(k, 2)]
    return jnp.concatenate(order, axis=-1)


def disarrange(a):
    cut = lambda i: a[..., i * HD : (i + 1) * HD]
    join = lambda *ids: jnp.concatenate([cut(i) for i in ids], axis=-1)
    return join(4, 5, 3), join(6, 7, 11), join(8, 9, 10), join(0, 1, 2)


def shards(
    tokens, seg_ids, counts, gain_attn, gain_ffn, w_qkv, dconv_kernel, w_out, w_up, w_down, grad_out
):
    rows, width = tokens.shape
    n_mp = lax.axis_size("mp")
    n_batch = lax.axis_size("batch")
    part = width // n_mp
    shard = w_qkv.shape[0]
    fits = (
        rows % SEQ_MAX == 0 and part == 3 * HD and width == 4 * part and shard % 16 == 0
        and w_up.shape[1] == width and seg_ids.shape[0] == n_mp * rows and shard % 32 == 0 and n_batch % 2 == 0
        and rows + HALO == width
    )
    if not fits:
        return shards_plain(
            tokens, seg_ids, counts, gain_attn, gain_ffn, w_qkv, dconv_kernel, w_out, w_up, w_down, grad_out
        )
    own_start = lax.axis_index("mp") * rows
    piece_a = arrange(w_qkv[:, 0], w_qkv[:, 1], w_qkv[:, 2], w_out.T)
    pieces = jnp.stack([piece_a, w_up, w_down.T])
    taps = lax.all_gather(dconv_kernel, "mp", axis=0, tiled=False)
    zero = jnp.zeros_like(taps[:, 0])
    kernel = arrange(taps[:, 0], taps[:, 1], taps[:, 2], zero)[..., BLK:]
    seg_pad = jnp.concatenate([jnp.full((HALO,), -1, jnp.int32), seg_ids])
    seg = lax.dynamic_slice_in_dim(seg_pad, own_start, HALO + rows, 0).astype(F32)
    slot = own_start - HALO + lax.iota(jnp.int32, HALO + rows)
    cols = jnp.stack(
        [
            (seg == later(seg, 1)).astype(F32).at[0].set(0.0),
            (seg == later(seg, 2)).astype(F32).at[:2].set(0.0),
            seg,
            (slot < counts[0]).astype(F32),
        ],
        axis=1,
    )
    gains = jnp.stack([gain_attn, gain_ffn])
    layer_out, grad_tokens, own, small = layer_call(pieces, tokens, grad_out, cols, seg[None, HALO:], gains, kernel)
    first, second, third, _ = disarrange(small[:3])
    piece = part // n_batch
    at_piece = lax.axis_index("batch") * piece
    taps_grad = lax.dynamic_slice_in_dim(jnp.stack([first, second, third]), at_piece, piece, 2)
    gain_grads = lax.dynamic_slice_in_dim(small[3:5], lax.axis_index("mp") * part + at_piece, piece, 1)
    q, k, v, o = disarrange(own[0])
    return (
        layer_out,
        grad_tokens,
        gain_grads[0],
        gain_grads[1],
        jnp.stack([q, k, v], axis=1),
        taps_grad,
        o.T,
        own[1],
        own[2].T,
    )


def solution(mesh):
    in_specs = (
        P(("batch", "mp"), None),
        P("batch"),
        P("batch"),
        P(),
        P(),
        P("batch", None, "mp"),
        P(None, None, "mp"),
        P("mp", "batch"),
        P("batch", "mp"),
        P("mp", "batch"),
        P(("batch", "mp"), None),
    )
    out_specs = (
        P(("batch", "mp"), None),
        P(("batch", "mp"), None),
        P(("mp", "batch")),
        P(("mp", "batch")),
        P("batch", None, "mp"),
        P(None, None, ("mp", "batch")),
        P("mp", "batch"),
        P("batch", "mp"),
        P("mp", "batch"),
    )
    return jax.shard_map(shards, mesh=mesh, in_specs=in_specs, out_specs=out_specs, check_vma=False)
```

```python
import jax
import jax.numpy as jnp
from jax import lax
from jax.experimental import pallas as pl
from jax.experimental.pallas import tpu as pltpu
from jax.sharding import PartitionSpec as P

HD = 64
SEQ_MAX = 256
PAD = 16
EPSILON = 1e-06
MASKED = -1e30
F32 = jnp.float32
BF16 = jnp.bfloat16


def nt(left, right):
    return lax.dot_general(left, right, (((1,), (1,)), ((), ())), preferred_element_type=F32)


def nn(left, right):
    return lax.dot_general(left, right, (((1,), (0,)), ((), ())), preferred_element_type=F32)


def tn(left, right):
    return lax.dot_general(left, right, (((0,), (0,)), ((), ())), preferred_element_type=F32)


def head_mask(values, head):
    lane = lax.broadcasted_iota(jnp.int32, values.shape, 1)
    return jnp.where((lane >= head * HD) & (lane < (head + 1) * HD), values, jnp.zeros_like(values))


def attend_kernel(q_ref, k_ref, v_ref, seg_key_ref, seg_query_ref, out_ref, prob_ref, bias_ref):
    tile = SEQ_MAX
    tiles = q_ref.shape[0] // tile

    @pl.when(pl.program_id(0) == 0)
    def _():
        for at in range(tiles):
            key = lax.broadcasted_iota(jnp.int32, (2 * tile, tile), 0)
            query = lax.broadcasted_iota(jnp.int32, (2 * tile, tile), 1) + tile
            same = seg_key_ref[at * tile : (at + 2) * tile, :] == seg_query_ref[:, at * tile : (at + 1) * tile]
            bias_ref[at] = jnp.where(same & (key <= query), 0.0, MASKED).astype(F32)

    for at in range(tiles):
        keys = k_ref[at * tile : (at + 2) * tile, :]
        values = v_ref[at * tile : (at + 2) * tile, :]
        queries = q_ref[at * tile : (at + 1) * tile, :] * jnp.asarray(HD**-0.5, BF16)
        outs = []
        for head in range(2):
            scores = nt(keys, head_mask(queries, head)) + bias_ref[at]
            expo = jnp.exp(scores - jnp.max(scores, axis=0, keepdims=True))
            prob = (expo * (1.0 / jnp.sum(expo, axis=0, keepdims=True))).astype(BF16)
            prob_ref[0, at, head] = prob
            outs.append(tn(head_mask(values, head), prob))
        out_ref[at * tile : (at + 1) * tile, :] = (outs[0] + outs[1]).T.astype(BF16)


def attend_back_kernel(q_ref, k_ref, v_ref, grad_ref, prob_ref, dq_ref, dk_ref, dv_ref):
    tile = SEQ_MAX
    tiles = q_ref.shape[0] // tile
    dk_ref[...] = jnp.zeros_like(dk_ref)
    dv_ref[...] = jnp.zeros_like(dv_ref)
    for at in range(tiles):
        span = slice(at * tile, (at + 2) * tile)
        keys = k_ref[span, :]
        values = v_ref[span, :]
        queries = q_ref[at * tile : (at + 1) * tile, :] * jnp.asarray(HD**-0.5, BF16)
        grads = grad_ref[at * tile : (at + 1) * tile, :]
        dq = 0.0
        for head in range(2):
            prob = prob_ref[0, at, head]
            grad_head = head_mask(grads, head)
            grad_prob = nt(values, grad_head)
            wide = prob.astype(F32)
            inner = wide * grad_prob
            grad_scores = (inner - wide * jnp.sum(inner, axis=0, keepdims=True)).astype(BF16)
            dv_ref[span, :] += nn(prob, grad_head)
            dk_ref[span, :] += nn(grad_scores, head_mask(queries, head))
            dq = dq + tn(head_mask(keys, head), grad_scores)
        dq_ref[at * tile : (at + 1) * tile, :] = (dq * HD**-0.5).T


def attend(queries, keys, values, seg_key, seg_query):
    rows, width = queries.shape
    span = keys.shape[0]
    tiles = rows // SEQ_MAX
    wide = 2 * HD
    return pl.pallas_call(
        attend_kernel,
        grid=(width // wide,),
        in_specs=[
            pl.BlockSpec((rows, wide), lambda i: (0, i)),
            pl.BlockSpec((span, wide), lambda i: (0, i)),
            pl.BlockSpec((span, wide), lambda i: (0, i)),
            pl.BlockSpec((span, 1), lambda i: (0, 0)),
            pl.BlockSpec((1, rows), lambda i: (0, 0)),
        ],
        out_specs=[
            pl.BlockSpec((rows, wide), lambda i: (0, i)),
            pl.BlockSpec((1, tiles, 2, 2 * SEQ_MAX, SEQ_MAX), lambda i: (i, 0, 0, 0, 0)),
        ],
        out_shape=[
            jax.ShapeDtypeStruct((rows, width), BF16),
            jax.ShapeDtypeStruct((width // wide, tiles, 2, 2 * SEQ_MAX, SEQ_MAX), BF16),
        ],
        scratch_shapes=[pltpu.VMEM((tiles, 2 * SEQ_MAX, SEQ_MAX), F32)],
        name="attend",
    )(queries, keys, values, seg_key[:, None], seg_query[None, :])


def attend_back(queries, keys, values, grads, prob):
    rows, width = queries.shape
    span = keys.shape[0]
    tiles = rows // SEQ_MAX
    wide = 2 * HD
    return pl.pallas_call(
        attend_back_kernel,
        grid=(width // wide,),
        in_specs=[
            pl.BlockSpec((rows, wide), lambda i: (0, i)),
            pl.BlockSpec((span, wide), lambda i: (0, i)),
            pl.BlockSpec((span, wide), lambda i: (0, i)),
            pl.BlockSpec((rows, wide), lambda i: (0, i)),
            pl.BlockSpec((1, tiles, 2, 2 * SEQ_MAX, SEQ_MAX), lambda i: (i, 0, 0, 0, 0)),
        ],
        out_specs=[
            pl.BlockSpec((rows, wide), lambda i: (0, i)),
            pl.BlockSpec((span, wide), lambda i: (0, i)),
            pl.BlockSpec((span, wide), lambda i: (0, i)),
        ],
        out_shape=[
            jax.ShapeDtypeStruct((rows, width), F32),
            jax.ShapeDtypeStruct((span, width), F32),
            jax.ShapeDtypeStruct((span, width), F32),
        ],
        name="attend_back",
    )(queries, keys, values, grads, prob)


def rms(values):
    return lax.rsqrt(jnp.mean(values * values, axis=-1, keepdims=True) + EPSILON)


def rms_back(grad, gain, hat, scale):
    scaled = grad * gain
    return scale * (scaled - hat * jnp.mean(scaled * hat, axis=-1, keepdims=True))


def later(values, by):
    return jnp.concatenate([jnp.zeros((by,) + values.shape[1:], values.dtype), values[:-by]], axis=0)


def sooner(values, by):
    return jnp.concatenate([values[by:], jnp.zeros((by,) + values.shape[1:], values.dtype)], axis=0)


def shards_plain(
    tokens, seg_ids, counts, gain_attn, gain_ffn, w_qkv, dconv_kernel, w_out, w_up, w_down, grad_out
):
    rows, width = tokens.shape
    halo = SEQ_MAX + PAD
    n_mp = lax.axis_size("mp")
    n_batch = lax.axis_size("batch")
    part = width // n_mp
    ff = w_up.shape[1] * n_mp
    own_start = lax.axis_index("mp") * rows

    packed = jnp.concatenate(
        [w_qkv.reshape(w_qkv.shape[0], -1), w_out.T, w_up, w_down.T], axis=1
    )
    full = lax.all_gather(packed, ("batch", "mp"), axis=0, tiled=False)
    full = full.reshape((n_batch, n_mp) + packed.shape).transpose(0, 2, 1, 3).reshape(width, n_mp, -1)
    cuts = (3 * part, 4 * part, 4 * part + w_up.shape[1])
    full_qkv = full[:, :, : cuts[0]].reshape(width, n_mp, 3, part).transpose(0, 2, 1, 3).reshape(width, 3 * width)
    full_out = full[:, :, cuts[0] : cuts[1]].reshape(width, width)
    full_up = full[:, :, cuts[1] : cuts[2]].reshape(width, ff)
    full_down = full[:, :, cuts[2] :].reshape(width, ff)
    kernel = lax.all_gather(dconv_kernel, "mp", axis=2, tiled=True).transpose(1, 0, 2).reshape(3, 3 * width)

    back = [(i, i + 1) for i in range(n_mp - 1)]
    tok_halo = lax.ppermute(tokens[rows - halo :], "mp", back)
    ext = jnp.concatenate([tok_halo, tokens], axis=0).astype(F32)
    seg_pad = jnp.concatenate([jnp.full((halo,), -1, jnp.int32), seg_ids])
    seg = lax.dynamic_slice_in_dim(seg_pad, own_start, halo + rows, 0)
    same_one = (seg == later(seg, 1)).astype(F32)[:, None]
    same_two = (seg == later(seg, 2)).astype(F32)[:, None]
    slot = own_start + lax.iota(jnp.int32, rows)
    filled = (slot < counts[0]).astype(F32)[:, None]

    scale_one = rms(ext)
    hat_one = ext * scale_one
    normed = (hat_one * gain_attn).astype(BF16)
    projected = nn(normed, full_qkv)
    mixed = (
        kernel[0] * projected
        + kernel[1] * same_one * later(projected, 1)
        + kernel[2] * same_two * later(projected, 2)
    ).astype(BF16)
    queries = mixed[halo:, :width]
    keys = mixed[PAD:, width : 2 * width]
    values = mixed[PAD:, 2 * width :]
    heads, prob = attend(queries, keys, values, seg[PAD:], seg[halo:])
    residual = ext[halo:] + filled * nn(heads, full_out.T if False else full_out.T)
    scale_two = rms(residual)
    hat_two = residual * scale_two
    normed_two = (hat_two * gain_ffn).astype(BF16)
    up = jax.nn.relu(nn(normed_two, full_up))
    hidden = (up * up).astype(BF16)
    layer_out = (residual + filled * nt(hidden, full_down)).astype(BF16)

    grad = grad_out.astype(F32)
    grad_ffn = (filled * grad).astype(BF16)
    grad_up = (nn(grad_ffn, full_down) * 2.0 * up).astype(BF16)
    grad_w_down = tn(grad_ffn, hidden)
    grad_w_up = tn(normed_two, grad_up)
    grad_normed_two = nt(grad_up, full_up)
    grad_resid = grad + rms_back(grad_normed_two, gain_ffn, hat_two, scale_two)
    grad_gain_ffn = jnp.sum(grad_normed_two * hat_two, axis=0)
    grad_attn = (filled * grad_resid).astype(BF16)
    grad_w_out = tn(grad_attn, heads)
    grad_heads = nn(grad_attn, full_out).astype(BF16)
    dq, dk, dv = attend_back(queries, keys, values, grad_heads, prob)
    grad_mixed = jnp.concatenate(
        [
            jnp.pad(dq, ((halo, 0), (0, 0))),
            jnp.pad(dk, ((PAD, 0), (0, 0))),
            jnp.pad(dv, ((PAD, 0), (0, 0))),
        ],
        axis=1,
    )
    one = grad_mixed * same_one
    two = grad_mixed * same_two
    grad_kernel = jnp.stack(
        [
            jnp.sum(grad_mixed * projected, axis=0),
            jnp.sum(one * later(projected, 1), axis=0),
            jnp.sum(two * later(projected, 2), axis=0),
        ]
    )
    grad_proj = (
        kernel[0] * grad_mixed + kernel[1] * sooner(one, 1) + kernel[2] * sooner(two, 2)
    ).astype(BF16)
    grad_w_qkv = tn(normed, grad_proj)
    grad_normed = nt(grad_proj, full_qkv)
    ahead = [(i + 1, i) for i in range(n_mp - 1)]
    passed = lax.ppermute(grad_normed[:halo].astype(BF16), "mp", ahead).astype(F32)
    own_normed = grad_normed[halo:] + jnp.pad(passed, ((rows - halo, 0), (0, 0)))
    grad_tokens = grad_resid + rms_back(own_normed, gain_attn, hat_one[halo:], scale_one[halo:])
    grad_gain_attn = jnp.sum(own_normed * hat_one[halo:], axis=0)

    shard = packed.shape[0]
    grads = jnp.concatenate(
        [
            grad_w_qkv.astype(BF16).reshape(width, 3, n_mp, part).transpose(0, 2, 1, 3).reshape(width, n_mp, -1),
            grad_w_out.astype(BF16).reshape(width, n_mp, -1),
            grad_w_up.astype(BF16).reshape(width, n_mp, -1),
            grad_w_down.astype(BF16).reshape(width, n_mp, -1),
        ],
        axis=2,
    )
    grads = grads.reshape(n_batch, shard, n_mp, -1).transpose(0, 2, 1, 3).reshape(n_batch * n_mp, shard, -1)
    own = lax.psum_scatter(grads, ("batch", "mp"), scatter_dimension=0, tiled=False).astype(F32)
    small = jnp.concatenate(
        [grad_kernel.reshape(3, 3, width).transpose(1, 0, 2).reshape(9, width), grad_gain_attn[None], grad_gain_ffn[None]]
    )
    piece = width // (n_mp * n_batch)
    small = small.reshape(11, n_mp * n_batch, piece).transpose(1, 0, 2)
    small = lax.psum_scatter(small, ("mp", "batch"), scatter_dimension=0, tiled=False)
    return (
        layer_out,
        grad_tokens,
        small[9],
        small[10],
        own[:, : cuts[0]].reshape(shard, 3, part),
        small[:9].reshape(3, 3, piece),
        own[:, cuts[0] : cuts[1]].T,
        own[:, cuts[1] : cuts[2]],
        own[:, cuts[2] :].T,
    )


HALO = SEQ_MAX
BLK = 128
HEADS = ((1, 2, 3, False, False, 0), (1, 2, 3, True, True, 0), (0, 4, 4, True, False, 1))
COLUMNS = 5 * BLK


def blk(index):
    return slice(index * BLK, (index + 1) * BLK)


def half_of(values, upper):
    lane = lax.broadcasted_iota(jnp.int32, values.shape, 1)
    keep = (lane >= HD) if upper else (lane < HD)
    return jnp.where(keep, values, jnp.zeros_like(values))


def rows_loop(total, size, body):
    def one(i, carry):
        body(pl.ds(pl.multiple_of(i * size, size), size))
        return carry

    lax.fori_loop(0, total // size, one, 0)


def parts_loop(count, body):
    def one(i, carry):
        body(i)
        return carry

    lax.fori_loop(0, count, one, 0)


MESH = pl.DeviceIdType.MESH


def meet_all():
    barrier = pltpu.get_barrier_semaphore()
    others = 0
    for axis in ("batch", "mp"):
        size = lax.axis_size(axis)
        for by in range(1, size):
            other = lax.rem(lax.axis_index(axis) + by, size)
            pl.semaphore_signal(barrier, inc=1, device_id={axis: other}, device_id_type=MESH)
        others += size - 1
    pl.semaphore_wait(barrier, others)


class Place:
    def __init__(self):
        self.b = lax.axis_index("batch")
        self.m = lax.axis_index("mp")
        self.zs = lax.axis_size("batch") // 2
        self.z = self.b // 2
        self.y = lax.rem(self.b, 2)

    def behind(self, k):
        return lax.rem(self.z + self.zs - k, self.zs) * 2

    def ahead(self, k):
        return lax.rem(self.z + k, self.zs) * 2

    def flip_x(self):
        return lax.rem(self.m + 2, 4)

    def flip_core(self, m):
        return m + 1 - 2 * lax.rem(m, 2)


class Gather:
    def __init__(self, pieces, w, send_sems, recv_sems, own_sems):
        self.pieces, self.w, self.send, self.recv, self.own = pieces, w, send_sems, recv_sems, own_sems
        self.at = Place()
        self.shard = pieces.shape[1]
        self.half = self.shard // 2

    def spot(self, p, c, k, j, core=False):
        at = self.at
        cross_y = j in ((1, 3) if c == 0 else (2, 3))
        cross_x = j in ((2, 3) if c == 0 else (1, 3))
        b = at.behind(k) + (1 - at.y if cross_y else at.y)
        m = at.flip_x() if cross_x else at.m
        m = at.flip_core(m) if core else m
        half = slice(c * self.half, (c + 1) * self.half)
        return self.w.at[p, m // 2, lax.rem(m, 2), b // 2, lax.rem(b, 2), half, :]

    def copy(self, p, c, k, j, number, target, core=False):
        own = self.pieces.at[p, c * self.half : (c + 1) * self.half, :]
        return pltpu.make_async_remote_copy(
            own if (k, j) == (0, 0) else self.spot(p, c, k, j),
            self.spot(p, c, k, j),
            self.send.at[p, c, number],
            self.recv.at[p, c, number],
            device_id=target,
            device_id_type=MESH,
        )

    def to(self, axis):
        at = self.at
        return {"batch": at.z * 2 + 1 - at.y} if axis == "y" else {"mp": at.flip_x()}

    def along_z(self, p, c):
        return [
            self.copy(p, c, 0, 0, by - 1, {"batch": self.at.ahead(by) + self.at.y}) for by in range(1, self.at.zs)
        ]

    def hops(self, p, c, k, j):
        zs = self.at.zs
        axes = ("y", "x") if c == 0 else ("x", "y")
        out = []
        if j == 0:
            out.append(self.copy(p, c, k, j, zs - 1 + k, self.to(axes[0])))
        if j in (0, 1):
            out.append(self.copy(p, c, k, j, 2 * zs - 1 + 2 * k + j, self.to(axes[1])))
        out.append(self.copy(p, c, k, j, 4 * zs - 1 + 4 * k + j, {"mp": self.at.flip_core(self.at.m)}))
        return out

    def arrived(self, p, c, k, j):
        zs = self.at.zs
        number = (k - 1, zs - 1 + k, 2 * zs - 1 + 2 * k, 2 * zs + 2 * k)[j]
        self.wait(p, c, number, self.spot(p, c, k, j))

    def wait(self, p, c, number, ref):
        pltpu.make_async_copy(ref, ref, self.recv.at[p, c, number]).wait()

    def keep(self, p):
        at = self.at
        own = self.w.at[p, at.m // 2, lax.rem(at.m, 2), at.z, at.y]
        return pltpu.make_async_copy(self.pieces.at[p], own, self.own.at[p])

    def begin_z(self, p):
        self.keep(p).start()
        copies = [self.along_z(p, c) for c in range(2)]
        for by in range(self.at.zs - 1):
            for c in range(2):
                copies[c][by].start()

    def begin(self, p):
        for c in range(2):
            for hop in self.hops(p, c, 0, 0):
                hop.start()

    def relay(self, p, j):
        for k in range(self.at.zs):
            for c in range(2):
                if (k, j) != (0, 0):
                    self.arrived(p, c, k, j)
                    for hop in self.hops(p, c, k, j):
                        hop.start()

    def finish(self, p):
        self.keep(p).wait()
        for k in range(self.at.zs):
            for j in range(4):
                for c in range(2):
                    self.wait(p, c, 4 * self.at.zs - 1 + 4 * k + j, self.spot(p, c, k, j, core=True))

    def drain(self, p):
        for c in range(2):
            for copy in self.along_z(p, c):
                copy.wait_send()
            for k in range(self.at.zs):
                for j in range(4):
                    for hop in self.hops(p, c, k, j):
                        hop.wait_send()


class Reduce:
    def __init__(self, w, one, two, three, four, one_sems, sems):
        self.w, self.one, self.two, self.three, self.four, self.one_sems, self.sems = (
            w, one, two, three, four, one_sems, sems
        )
        self.at = Place()
        self.x = self.at.m // 2
        self.core = lax.rem(self.at.m, 2)
        self.half = w.shape[5] // 2

    def z(self, k):
        return self.at.ahead(k) // 2

    def lanes(self, c):
        return slice(c * self.half, (c + 1) * self.half)

    def remote(self, source, target, sems, number, device):
        return pltpu.make_async_remote_copy(
            source, target, sems.at[(0,) + number], sems.at[(1,) + number], device_id=device, device_id_type=MESH
        )

    def first(self, p, x):
        other = {"mp": self.at.flip_core(self.at.m)}
        return self.remote(self.w.at[p, x, 1 - self.core], self.one.at[p, x], self.one_sems, (p, x), other)

    def second(self, p, k, c):
        z, at = self.z(k), self.at
        if c == 0:
            source, device = self.w.at[p, 1 - self.x, self.core, z, :, self.lanes(0), :], {"mp": at.flip_x()}
        else:
            source = self.w.at[p, :, self.core, z, 1 - at.y, self.lanes(1), :]
            device = {"batch": at.z * 2 + 1 - at.y}
        return self.remote(source, self.two.at[p, k, c], self.sems, (p, k, c), device)

    def third(self, p, k, c):
        z, at = self.z(k), self.at
        if c == 0:
            source = self.w.at[p, self.x, self.core, z, 1 - at.y, self.lanes(0), :]
            device = {"batch": at.z * 2 + 1 - at.y}
        else:
            source, device = self.w.at[p, 1 - self.x, self.core, z, at.y, self.lanes(1), :], {"mp": at.flip_x()}
        return self.remote(source, self.three.at[p, k, c], self.sems, (p, k, 2 + c), device)

    def fourth(self, p, k, c):
        at = self.at
        source = self.w.at[p, self.x, self.core, self.z(k), at.y, self.lanes(c), :]
        return self.remote(source, self.four.at[p, k - 1, c], self.sems, (p, k, 4 + c), {"batch": at.ahead(k) + at.y})

    def start(self, p):
        for x in range(2):
            self.first(p, x).start()

    def met(self, p):
        for x in range(2):
            self.first(p, x).wait_recv()

    def step_one(self, p, k):
        z = self.z(k)
        for x in range(2):
            self.w[p, x, self.core, z] += self.one[p, x, z]
        for c in range(2):
            self.second(p, k, c).start()

    def step_two(self, p, k):
        z, at = self.z(k), self.at
        self.second(p, k, 0).wait_recv()
        for y in range(2):
            self.w[p, self.x, self.core, z, y, self.lanes(0), :] += self.two[p, k, 0, y]
        self.third(p, k, 0).start()
        self.second(p, k, 1).wait_recv()
        for x in range(2):
            self.w[p, x, self.core, z, at.y, self.lanes(1), :] += self.two[p, k, 1, x]
        self.third(p, k, 1).start()

    def step_three(self, p, k):
        z, at = self.z(k), self.at
        for c in range(2):
            self.third(p, k, c).wait_recv()
            self.w[p, self.x, self.core, z, at.y, self.lanes(c), :] += self.three[p, k, c]
            if k:
                self.fourth(p, k, c).start()

    def step_four(self, p, out):
        for c in range(2):
            total = self.w[p, self.x, self.core, self.at.z, self.at.y, self.lanes(c), :].astype(F32)
            for k in range(1, self.at.zs):
                self.fourth(p, k, c).wait_recv()
                total = total + self.four[p, k - 1, c].astype(F32)
            out[p, self.lanes(c), :] = total

    def drain(self, p):
        for x in range(2):
            self.first(p, x).wait_send()
        for k in range(self.at.zs):
            for c in range(2):
                self.second(p, k, c).wait_send()
                self.third(p, k, c).wait_send()
                if k:
                    self.fourth(p, k, c).wait_send()


class Small:
    def __init__(self, source, one, two, three, sums, sems):
        self.source, self.one, self.two, self.three, self.sums, self.sems = source, one, two, three, sums, sems
        self.at = Place()
        self.x = self.at.m // 2
        self.core = lax.rem(self.at.m, 2)
        self.count = lax.axis_size("batch")

    def remote(self, source, target, number, device):
        return pltpu.make_async_remote_copy(
            source, target, self.sems.at[0, number], self.sems.at[1, number], device_id=device, device_id_type=MESH
        )

    def core_copy(self, x):
        device = {"mp": self.at.flip_core(self.at.m)}
        return self.remote(self.source.at[x * 2 + 1 - self.core], self.one.at[x], x, device)

    def x_copy(self):
        return self.remote(self.sums.at[1 - self.x], self.two, 2, {"mp": self.at.flip_x()})

    def far_copy(self, by):
        other = lax.rem(self.at.b + by, self.count)
        return self.remote(self.sums.at[self.x], self.three.at[by - 1], 2 + by, {"batch": other})

    def begin(self):
        for x in range(2):
            self.core_copy(x).start()

    def middle(self):
        for x in range(2):
            self.core_copy(x).wait_recv()
            self.sums[x] = self.source[x * 2 + self.core] + self.one[x]
        self.x_copy().start()

    def later(self):
        self.x_copy().wait_recv()
        self.sums[self.x] += self.two[...]
        for by in range(1, self.count):
            self.far_copy(by).start()

    def finish(self, out):
        total = self.sums[self.x]
        for by in range(1, self.count):
            self.far_copy(by).wait_recv()
            total = total + self.three[by - 1]
        out[...] = total
        for x in range(2):
            self.core_copy(x).wait_send()
        self.x_copy().wait_send()
        for by in range(1, self.count):
            self.far_copy(by).wait_send()


def layer_kernel(
    pieces_ref, tok_ref, grad_ref, cols_ref, seg_row_ref, gains_ref, taps_ref,
    out_ref, tokens_out, own_out, small_out,
    w, ext_ref, normed, proj, mixed, prob, heads, bias, wide, acc, own_ref, normed_two,
    gffn_t, two_t, hidden, upper, one, two, three, four, sent, passed,
    small_ref, s_sums, s_one, s_two, s_three, kernel_ref,
    send_sems, recv_sems, own_sems, halo_sems, one_sems, sems, small_sems, taps_sems,
):
    parts = w.shape[1] * w.shape[2]
    rows, width = tokens_out.shape
    span = HALO + rows
    tiles = rows // SEQ_MAX
    tile = SEQ_MAX
    resid = tokens_out
    me = lax.axis_index("mp")
    pull = Gather(pieces_ref, w, send_sems, recv_sems, own_sems)
    push = Reduce(w, one, two, three, four, one_sems, sems)
    small = Small(small_ref, s_one, s_two, s_three, s_sums, small_sems)
    zs = push.at.zs
    ks = [*range(1, zs), 0]

    def weight(piece, m):
        return w[piece, m // 2, lax.rem(m, 2)].reshape(width, width)

    def store(piece, m, lanes, value):
        w[piece, m // 2, lax.rem(m, 2), :, :, :, lanes] = value.reshape(zs, 2, width // (2 * zs), value.shape[1])

    def lanes_of(piece, m, lanes):
        value = w[piece, m // 2, lax.rem(m, 2), :, :, :, lanes]
        return value.reshape(width, value.shape[3])

    def neighbour(source, target, first, by):
        return pltpu.make_async_remote_copy(
            source, target, halo_sems.at[first], halo_sems.at[first + 1],
            device_id={"mp": lax.rem(me + by, parts)}, device_id_type=MESH,
        )

    def taps_copy(by):
        return pltpu.make_async_remote_copy(
            taps_ref, kernel_ref.at[me], taps_sems.at[0, by - 1], taps_sems.at[1, by - 1],
            device_id={"mp": lax.rem(me + by, parts)}, device_id_type=MESH,
        )

    meet_all()
    for by in range(1, parts):
        taps_copy(by).start()
    kernel_ref[me] = taps_ref[...]
    pull.begin_z(0)
    pull.begin(0)
    pass_on = neighbour(tok_ref.at[rows - HALO :], ext_ref.at[:HALO], 0, 1)
    pass_on.start()
    pull.begin_z(1)
    pull.begin_z(2)
    ext_ref[HALO:, :] = tok_ref[...]

    gain_one = gains_ref[0:1, :]
    gain_two = gains_ref[1:2, :]

    def norm_one(at):
        values = ext_ref[at, :].astype(F32)
        normed[at, :] = (values * rms(values) * gain_one).astype(BF16)

    pass_on.wait()
    for by in range(1, parts):
        other = kernel_ref.at[lax.rem(me + parts - by, parts)]
        pltpu.make_async_copy(other, other, taps_sems.at[1, by - 1]).wait()
        taps_copy(by).wait_send()
    rows_loop(span, 128, norm_one)
    for at in range(tiles):
        key = lax.broadcasted_iota(jnp.int32, (2 * tile, tile), 0)
        query = lax.broadcasted_iota(jnp.int32, (2 * tile, tile), 1) + tile
        seg_key = cols_ref[at * tile : (at + 2) * tile, 2:3]
        same = seg_key == seg_row_ref[0:1, at * tile : (at + 1) * tile]
        bias[at] = jnp.where(same & (key <= query), 0.0, MASKED).astype(BF16)
    acc[...] = jnp.zeros_like(acc)

    def forward(m):
        wide[...] = nn(normed[...], lanes_of(0, m, slice(BLK, width)))
        for c in range(5):
            source = wide[:, blk(c)]
            proj[m, :, blk(c)] = source.astype(BF16)
            mixed[m, :, blk(c)] = (
                kernel_ref[m, 0:1, blk(c)] * source
                + kernel_ref[m, 1:2, blk(c)] * (cols_ref[:, 0:1] * pltpu.roll(source, 1, 0))
                + kernel_ref[m, 2:3, blk(c)] * (cols_ref[:, 1:2] * pltpu.roll(source, 2, 0))
            ).astype(BF16)
        for at in range(tiles):
            keys_at = slice(at * tile, (at + 2) * tile)
            query_at = slice(HALO + at * tile, HALO + (at + 1) * tile)
            outs = []
            for h, (qb, kb, vb, qk_upper, v_upper, _) in enumerate(HEADS):
                queries = half_of(mixed[m, query_at, blk(qb)], qk_upper) * jnp.asarray(HD**-0.5, BF16)
                scores = nt(mixed[m, keys_at, blk(kb)], queries) + bias[at].astype(F32)
                expo = jnp.exp(scores - jnp.max(scores, axis=0, keepdims=True))
                share = (expo * (1.0 / jnp.sum(expo, axis=0, keepdims=True))).astype(BF16)
                prob[m, at, h] = share
                outs.append(tn(half_of(mixed[m, keys_at, blk(vb)], v_upper), share))
            own_at = slice(at * tile, (at + 1) * tile)
            heads[m, own_at, blk(0)] = (outs[0] + outs[1]).T.astype(BF16)
            heads[m, own_at, blk(1)] = outs[2].T.astype(BF16)
        acc[...] += nt(heads[m], lanes_of(0, m, slice(0, 2 * BLK)))

        @pl.when(m == 1)
        def _():
            pull.relay(1, 1)
            pull.begin(2)
            pull.relay(2, 0)

        @pl.when(m == 2)
        def _():
            pull.relay(1, 2)
            pull.relay(1, 3)

    pull.relay(0, 0)
    pull.begin(1)
    for j in range(1, 4):
        pull.relay(0, j)
    pull.finish(0)
    pull.relay(1, 0)
    parts_loop(parts, forward)
    pull.relay(2, 1)

    def middle(at):
        values = ext_ref[pl.ds(at.start + HALO, at.size), :].astype(F32)
        filled = cols_ref[pl.ds(at.start + HALO, at.size), 3:4]
        value = values + filled * acc[at, :]
        resid[at, :] = value
        normed_two[at, :] = (value * rms(value) * gain_two).astype(BF16)
        out_ref[at, :] = (filled * grad_ref[at, :].astype(F32)).astype(BF16)

    rows_loop(rows, 128, middle)
    gffn = out_ref
    gffn_t[...] = gffn[...].T
    two_t[...] = normed_two[...].T
    normed[...] = normed[...].T
    normed_t = normed
    acc[...] = jnp.zeros_like(acc)
    own_ref[...] = jnp.zeros_like(own_ref)
    pull.relay(2, 2)
    pull.relay(2, 3)
    for p in (1, 2):
        pull.finish(p)
    for p in range(3):
        pull.drain(p)

    def feed(m):
        up = jnp.maximum(nn(normed_two[...], weight(1, m)), 0.0)
        upper[...] = (2.0 * up).astype(BF16)
        hidden[...] = (up * up).astype(BF16)
        acc[...] += nt(hidden[...], weight(2, m))
        upper[...] = (nn(gffn[...], weight(2, m)) * upper[...].astype(F32)).astype(BF16)
        store(2, m, slice(0, width), nn(gffn_t[...], hidden[...]).astype(BF16))
        own_ref[...] += nt(upper[...], weight(1, m))
        store(1, m, slice(0, width), nn(two_t[...], upper[...]).astype(BF16))

    parts_loop(parts, feed)
    push.start(2)
    push.start(1)

    small_ref[...] = jnp.zeros_like(small_ref)

    def turn(at):
        value = resid[at, :]
        filled = cols_ref[pl.ds(at.start + HALO, at.size), 3:4]
        scale = rms(value)
        hat = value * scale
        grad = own_ref[at, :]
        small_ref[0, 4:5, :] += jnp.sum(grad * hat, axis=0, keepdims=True)
        total = grad_ref[at, :].astype(F32) + rms_back(grad, gain_two, hat, scale)
        tokens_out[at, :] = total
        out_ref[at, :] = (value + filled * acc[at, :]).astype(BF16)
        normed_two[at, :] = (filled * total).astype(BF16)

    rows_loop(rows, 128, turn)
    gattn = normed_two
    two_t[...] = gattn[...].T
    own_ref[...] = jnp.zeros_like(own_ref)
    acc[...] = jnp.zeros_like(acc)

    def backward(m):
        @pl.when(m == 0)
        def _():
            push.met(2)
            for k in ks:
                push.step_one(2, k)

        @pl.when(m == 1)
        def _():
            push.met(1)
            push.step_one(1, ks[0])

        @pl.when(m == 2)
        def _():
            for k in ks:
                push.step_two(2, k)
            for k in ks[1:]:
                push.step_one(1, k)

        grads = nn(gattn[...], lanes_of(0, m, slice(0, 2 * BLK))).astype(BF16)
        hidden[:, : 2 * BLK] = grads
        wide[...] = jnp.zeros_like(wide)
        for at in range(tiles):
            keys_at = slice(at * tile, (at + 2) * tile)
            query_at = slice(HALO + at * tile, HALO + (at + 1) * tile)
            own_at = slice(at * tile, (at + 1) * tile)
            for h, (qb, kb, vb, qk_upper, v_upper, ob) in enumerate(HEADS):
                share = prob[m, at, h]
                grad_head = half_of(hidden[own_at, blk(ob)], v_upper)
                queries = half_of(mixed[m, query_at, blk(qb)], qk_upper) * jnp.asarray(HD**-0.5, BF16)
                grad_prob = nt(mixed[m, keys_at, blk(vb)], grad_head)
                broad = share.astype(F32)
                inner = broad * grad_prob
                grad_scores = (inner - broad * jnp.sum(inner, axis=0, keepdims=True)).astype(BF16)
                wide[keys_at, blk(vb)] += nn(share, grad_head)
                wide[keys_at, blk(kb)] += nn(grad_scores, queries)
                keys = half_of(mixed[m, keys_at, blk(kb)], qk_upper)
                wide[query_at, blk(qb)] += (tn(keys, grad_scores) * HD**-0.5).T
        for c in range(5):
            grad = wide[:, blk(c)]
            one = grad * cols_ref[:, 0:1]
            two = grad * cols_ref[:, 1:2]
            source = proj[m, :, blk(c)].astype(F32)
            small_ref[m, 0:1, blk(c + 1)] = jnp.sum(grad * source, axis=0, keepdims=True)
            small_ref[m, 1:2, blk(c + 1)] = jnp.sum(one * pltpu.roll(source, 1, 0), axis=0, keepdims=True)
            small_ref[m, 2:3, blk(c + 1)] = jnp.sum(two * pltpu.roll(source, 2, 0), axis=0, keepdims=True)
            mixed[m, :, blk(c)] = (
                kernel_ref[m, 0:1, blk(c)] * grad
                + kernel_ref[m, 1:2, blk(c)] * pltpu.roll(one, span - 1, 0)
                + kernel_ref[m, 2:3, blk(c)] * pltpu.roll(two, span - 2, 0)
            ).astype(BF16)
        own_ref[...] += nt(mixed[m, HALO:, :], lanes_of(0, m, slice(BLK, width)))
        acc[:HALO, :] += nt(mixed[m, :HALO, :], lanes_of(0, m, slice(BLK, width)))
        part = nn(two_t[...], heads[m])
        wide[...] = nn(normed_t[...], mixed[m])
        store(0, m, blk(0), part[:, blk(0)].astype(BF16))
        store(0, m, blk(1), (half_of(part[:, blk(1)], False) + half_of(wide[:, blk(0)], True)).astype(BF16))
        store(0, m, slice(2 * BLK, width), wide[:, BLK:].astype(BF16))

    parts_loop(parts, backward)
    push.start(0)
    sent[...] = acc[:HALO, :].astype(BF16)

    def gain_rows(at, grad):
        values = ext_ref[at, :].astype(F32)
        small_ref[0, 3:4, :] += jnp.sum(grad * (values * rms(values)), axis=0, keepdims=True)

    rows_loop(HALO, 128, lambda at: gain_rows(at, acc[at, :]))
    rows_loop(rows, 128, lambda at: gain_rows(pl.ds(at.start + HALO, at.size), own_ref[at, :]))
    for m in range(1, parts):
        small_ref[m, 3:5, :] = small_ref[0, 3:5, :]
    back_on = neighbour(sent, passed, 2, parts - 1)
    back_on.start()
    small.begin()
    for k in ks:
        push.step_three(2, k)
    push.met(0)
    for k in ks:
        push.step_two(1, k)
        push.step_one(0, k)
    small.middle()

    def last(at, extra):
        values = tok_ref[at, :].astype(F32)
        scale = rms(values)
        tokens_out[at, :] += rms_back(own_ref[at, :] + extra, gain_one, values * scale, scale)

    def end_rows(at):
        keep = jnp.where(me < parts - 1, 1.0, 0.0)
        last(pl.ds(at.start + rows - HALO, at.size), passed[at, :].astype(F32) * keep)

    rows_loop(rows - HALO, 128, lambda at: last(at, 0.0))
    small.later()
    back_on.wait()
    rows_loop(HALO, 128, end_rows)
    for k in ks:
        push.step_three(1, k)
    push.step_four(2, own_out)
    for k in ks:
        push.step_two(0, k)
    small.finish(small_out)
    for k in ks:
        push.step_three(0, k)
    push.step_four(1, own_out)
    push.step_four(0, own_out)
    for p in range(3):
        push.drain(p)


def layer_call(pieces, tokens, grad_out, cols, seg_row, gains, kernel):
    parts = lax.axis_size("mp")
    rows, width = grad_out.shape
    span = rows + HALO
    tiles = rows // SEQ_MAX
    zs = lax.axis_size("batch") // 2
    copies = 8 * zs - 1
    shard = width // (2 * zs)
    half = shard // 2
    vmem = pl.BlockSpec(memory_space=pltpu.VMEM)
    return pl.pallas_call(
        layer_kernel,
        in_specs=[vmem] * 7,
        out_specs=[vmem] * 4,
        out_shape=[
            jax.ShapeDtypeStruct((rows, width), BF16),
            jax.ShapeDtypeStruct((rows, width), F32),
            jax.ShapeDtypeStruct((3, shard, width), F32),
            jax.ShapeDtypeStruct((8, width), F32),
        ],
        scratch_shapes=[
            pltpu.VMEM((3, 2, 2, zs, 2, shard, width), BF16),
            pltpu.VMEM((span, width), BF16),
            pltpu.VMEM((span, width), BF16),
            pltpu.VMEM((parts, span, COLUMNS), BF16),
            pltpu.VMEM((parts, span, COLUMNS), BF16),
            pltpu.VMEM((parts, tiles, 3, 2 * SEQ_MAX, SEQ_MAX), BF16),
            pltpu.VMEM((parts, rows, 2 * BLK), BF16),
            pltpu.VMEM((tiles, 2 * SEQ_MAX, SEQ_MAX), BF16),
            pltpu.VMEM((span, COLUMNS), F32),
            pltpu.VMEM((rows, width), F32),
            pltpu.VMEM((rows, width), F32),
            pltpu.VMEM((rows, width), BF16),
            pltpu.VMEM((width, rows), BF16),
            pltpu.VMEM((width, rows), BF16),
            pltpu.VMEM((rows, width), BF16),
            pltpu.VMEM((rows, width), BF16),
            pltpu.VMEM((3, 2, zs, 2, shard, width), BF16),
            pltpu.VMEM((3, zs, 2, 2, half, width), BF16),
            pltpu.VMEM((3, zs, 2, half, width), BF16),
            pltpu.VMEM((3, zs - 1, 2, half, width), BF16),
            pltpu.VMEM((HALO, width), BF16),
            pltpu.VMEM((HALO, width), BF16),
            pltpu.VMEM((parts, 8, width), F32),
            pltpu.VMEM((2, 8, width), F32),
            pltpu.VMEM((2, 8, width), F32),
            pltpu.VMEM((8, width), F32),
            pltpu.VMEM((2 * zs - 1, 8, width), F32),
            pltpu.VMEM((parts, 8, COLUMNS), F32),
            pltpu.SemaphoreType.DMA((3, 2, copies)),
            pltpu.SemaphoreType.DMA((3, 2, copies)),
            pltpu.SemaphoreType.DMA((3,)),
            pltpu.SemaphoreType.DMA((4,)),
            pltpu.SemaphoreType.DMA((2, 3, 2)),
            pltpu.SemaphoreType.DMA((2, 3, zs, 6)),
            pltpu.SemaphoreType.DMA((2, 2 + 2 * zs)),
            pltpu.SemaphoreType.DMA((2, parts - 1)),
        ],
        compiler_params=pltpu.CompilerParams(
            vmem_limit_bytes=67043328, collective_id=0, has_side_effects=True
        ),
        name="layer",
    )(pieces, tokens, grad_out, cols, seg_row, gains, kernel)


def arrange(q, k, v, o):
    cut = lambda a, h: a[..., h * HD : (h + 1) * HD]
    order = [cut(o, 0), cut(o, 1), cut(o, 2), cut(q, 2), cut(q, 0), cut(q, 1)]
    order += [cut(k, 0), cut(k, 1), cut(v, 0), cut(v, 1), cut(v, 2), cut(k, 2)]
    return jnp.concatenate(order, axis=-1)


def disarrange(a):
    cut = lambda i: a[..., i * HD : (i + 1) * HD]
    join = lambda *ids: jnp.concatenate([cut(i) for i in ids], axis=-1)
    return join(4, 5, 3), join(6, 7, 11), join(8, 9, 10), join(0, 1, 2)


def shards(
    tokens, seg_ids, counts, gain_attn, gain_ffn, w_qkv, dconv_kernel, w_out, w_up, w_down, grad_out
):
    rows, width = tokens.shape
    n_mp = lax.axis_size("mp")
    n_batch = lax.axis_size("batch")
    part = width // n_mp
    shard = w_qkv.shape[0]
    fits = (
        rows % SEQ_MAX == 0 and part == 3 * HD and width == 4 * part and shard % 16 == 0
        and w_up.shape[1] == width and seg_ids.shape[0] == n_mp * rows and shard % 32 == 0 and n_batch % 2 == 0
        and rows + HALO == width
    )
    if not fits:
        return shards_plain(
            tokens, seg_ids, counts, gain_attn, gain_ffn, w_qkv, dconv_kernel, w_out, w_up, w_down, grad_out
        )
    own_start = lax.axis_index("mp") * rows
    piece_a = arrange(w_qkv[:, 0], w_qkv[:, 1], w_qkv[:, 2], w_out.T)
    pieces = jnp.stack([piece_a, w_up, w_down.T])
    zero = jnp.zeros_like(dconv_kernel[0])
    kernel = arrange(dconv_kernel[0], dconv_kernel[1], dconv_kernel[2], zero)[:, BLK:]
    kernel = jnp.pad(kernel, ((0, 5), (0, 0)))
    seg_pad = jnp.concatenate([jnp.full((HALO,), -1, jnp.int32), seg_ids])
    seg = lax.dynamic_slice_in_dim(seg_pad, own_start, HALO + rows, 0).astype(F32)
    slot = own_start - HALO + lax.iota(jnp.int32, HALO + rows)
    cols = jnp.stack(
        [
            (seg == later(seg, 1)).astype(F32).at[0].set(0.0),
            (seg == later(seg, 2)).astype(F32).at[:2].set(0.0),
            seg,
            (slot < counts[0]).astype(F32),
        ],
        axis=1,
    )
    gains = jnp.stack([gain_attn, gain_ffn])
    layer_out, grad_tokens, own, small = layer_call(pieces, tokens, grad_out, cols, seg[None, HALO:], gains, kernel)
    first, second, third, _ = disarrange(small[:3])
    piece = part // n_batch
    at_piece = lax.axis_index("batch") * piece
    taps_grad = lax.dynamic_slice_in_dim(jnp.stack([first, second, third]), at_piece, piece, 2)
    gain_grads = lax.dynamic_slice_in_dim(small[3:5], lax.axis_index("mp") * part + at_piece, piece, 1)
    q, k, v, o = disarrange(own[0])
    return (
        layer_out,
        grad_tokens,
        gain_grads[0],
        gain_grads[1],
        jnp.stack([q, k, v], axis=1),
        taps_grad,
        o.T,
        own[1],
        own[2].T,
    )


def solution(mesh):
    in_specs = (
        P(("batch", "mp"), None),
        P("batch"),
        P("batch"),
        P(),
        P(),
        P("batch", None, "mp"),
        P(None, None, "mp"),
        P("mp", "batch"),
        P("batch", "mp"),
        P("mp", "batch"),
        P(("batch", "mp"), None),
    )
    out_specs = (
        P(("batch", "mp"), None),
        P(("batch", "mp"), None),
        P(("mp", "batch")),
        P(("mp", "batch")),
        P("batch", None, "mp"),
        P(None, None, ("mp", "batch")),
        P("mp", "batch"),
        P("batch", "mp"),
        P("mp", "batch"),
    )
    return jax.shard_map(shards, mesh=mesh, in_specs=in_specs, out_specs=out_specs, check_vma=False)
```
